32 devices in a mesh: dp: 1 (over z), vp: 4 (over y), tp: 8 (over x, core).
Axes of the slice: x: 4, y: 4, z: 1, core: 2. Of those that a mesh axis runs over, the one named last changes fastest.
The devices are a block of a 4x4x8 slice.
Arguments:
- hidden: bfloat16 [64, 2048], P('dp', 'tp')
- lnf_gain: float32 [2048], P('tp')
- lnf_bias: float32 [2048], P('tp')
- emb_table: bfloat16 [250880, 2048], P('vp', 'tp')
- next_tok: int32 [64], P('dp')
- eln_gain: float32 [2048], P('tp')
- eln_bias: float32 [2048], P('tp')
Outputs:
- output 1: float32 [64, 250880], P('dp', ('vp', 'tp'))
- output 2: float32 [64], P('dp')
- output 3: bfloat16 [64, 2048], P('dp', 'tp')
All inputs are finite; a program needn't handle non-finite values.
Results may differ from the reference program's by a relative error of at most 0.001.
Values sent between devices are 32-bit elements.
A program may use at most 768 MiB of HBM per device.

```python
import jax
import jax.numpy as jnp

BATCH_ROWS = 64
D = 2048
VOCAB_SIZE = 250880
VP_BLOCKS = 4
HOT_COUNT = min(2, VP_BLOCKS)
NORM_EPS = 1e-5


def draw_tokens(key):
    key_hot, key_pick, key_any, key_sel, key_pos = jax.random.split(key, 5)
    block_len = VOCAB_SIZE // VP_BLOCKS
    hot_blocks = jax.random.permutation(key_hot, VP_BLOCKS)[:HOT_COUNT]
    hot_pick = jax.random.randint(key_pick, (BATCH_ROWS,), 0, HOT_COUNT)
    any_block = jax.random.randint(key_any, (BATCH_ROWS,), 0, VP_BLOCKS)
    use_hot = jax.random.randint(key_sel, (BATCH_ROWS,), 0, 4) < 3
    tok_block = jnp.where(use_hot, hot_blocks[hot_pick], any_block)
    tok_within = jax.random.randint(key_pos, (BATCH_ROWS,), 0, block_len)
    return (tok_block * block_len + tok_within).astype(jnp.int32)


def setup_inputs(seed: int = 0, part: int = 0) -> dict:
    shared_key, part_root = jax.random.split(jax.random.key(seed))
    part_key = jax.random.fold_in(part_root, part)
    key_hid, key_off, key_tok = jax.random.split(part_key, 3)
    key_tab, key_rowm, key_g1, key_b1, key_g2, key_b2 = jax.random.split(shared_key, 6)
    col_pos = jnp.arange(D, dtype=jnp.float32) / D
    hidden = jax.random.normal(key_hid, (BATCH_ROWS, D), jnp.float32) * (0.5 + 1.5 * col_pos)
    hidden = hidden + jax.random.normal(key_off, (BATCH_ROWS, 1), jnp.float32) * (1.0 + 2.0 * col_pos)
    tab_vals = jax.random.normal(key_tab, (VOCAB_SIZE, D), jnp.float32) * (0.5 + col_pos)
    tab_vals = (tab_vals + jax.random.normal(key_rowm, (VOCAB_SIZE, 1), jnp.float32)) * (D ** -0.5)
    return {
        "hidden": hidden.astype(jnp.bfloat16),
        "lnf_gain": 1.5 + 0.5 * jax.random.normal(key_g1, (D,), jnp.float32),
        "lnf_bias": 0.5 * jax.random.normal(key_b1, (D,), jnp.float32),
        "emb_table": tab_vals.astype(jnp.bfloat16),
        "next_tok": draw_tokens(key_tok),
        "eln_gain": 1.0 + 0.3 * jax.random.normal(key_g2, (D,), jnp.float32),
        "eln_bias": 0.5 * jax.random.normal(key_b2, (D,), jnp.float32),
    }


def layer_norm(rows_in, norm_gain, norm_bias):
    rows_f32 = rows_in.astype(jnp.float32)
    row_mean = jnp.mean(rows_f32, axis=-1, keepdims=True)
    row_var = jnp.mean(rows_f32 * rows_f32, axis=-1, keepdims=True) - row_mean * row_mean
    return (rows_f32 - row_mean) / jnp.sqrt(row_var + NORM_EPS) * norm_gain + norm_bias


def reference(hidden, lnf_gain, lnf_bias, emb_table, next_tok, eln_gain, eln_bias):
    normed = layer_norm(hidden, lnf_gain, lnf_bias).astype(jnp.bfloat16)
    logits = jnp.dot(normed, emb_table.T, preferred_element_type=jnp.float32)
    log_sum = jax.nn.logsumexp(logits, axis=-1)
    logprobs = logits - log_sum[:, None]
    tok_rows = jnp.take(emb_table, next_tok, axis=0)
    next_in = layer_norm(tok_rows, eln_gain, eln_bias).astype(jnp.bfloat16)
    return (logprobs, log_sum, next_in)
```

```python
import functools

import jax
import jax.numpy as jnp
from jax import lax
from jax.experimental import pallas as pl
from jax.experimental.pallas import tpu as pltpu
from jax.sharding import PartitionSpec as P

NORM_EPS = 1e-5
LANES = 128
CHUNK = 1024
DOT_COLS = 512
PICK = 1280
MESH_ID = pl.DeviceIdType.MESH


def _row_stats(x):
    sums = x[:, :LANES]
    squares = sums * sums
    for c in range(LANES, x.shape[1], LANES):
        part = x[:, c : c + LANES]
        sums = sums + part
        squares = squares + part * part
    both = jnp.concatenate([sums, squares], axis=0)
    return jnp.sum(both.T, axis=0, keepdims=True)


def _as_columns(row):
    return jnp.broadcast_to(row, (LANES, LANES)).T


def _normalize(x, total, gain, bias, full_width):
    rows = x.shape[0]
    cols = _as_columns(total)
    mean = cols[:rows] / full_width
    var = cols[rows : 2 * rows] / full_width - mean * mean
    rstd = lax.rsqrt(var + NORM_EPS)
    parts = []
    for c in range(0, x.shape[1], LANES):
        scaled = (x[:, c : c + LANES] - mean) * rstd
        parts.append(scaled * gain[:, c : c + LANES] + bias[:, c : c + LANES])
    return jnp.concatenate(parts, axis=1).astype(jnp.bfloat16)


def _head_kernel(
    tp_size, vp_size,
    hid, g1, b1, g2, b2, tok, emb,
    z_out, ls_out, nin_out,
    e_all, mine, from_peer, to_peer, ring, xn,
    top, acc, e_src, e_in, stat_src, stat_in, v_src, v_in,
    e_sem, peer_send, peer_recv, ring_send, ring_recv,
    stat_send, stat_recv, row_send, row_recv, v_send, v_recv, z_sem,
):
    rows, width = hid.shape
    full_width = width * tp_size
    vocab_rows = emb.shape[0]
    own_cols = vocab_rows // tp_size
    chips = tp_size // 2
    n_chunks = pl.cdiv(own_cols, CHUNK)
    half_chunks = n_chunks // 2
    half_cols = half_chunks * CHUNK
    tail = own_cols - (n_chunks - 1) * CHUNK
    tail_pad = pl.cdiv(tail, LANES) * LANES

    me = lax.axis_index("tp")
    my_vp = lax.axis_index("vp")
    chip = me // 2
    core = me % 2
    peer = 2 * chip + 1 - core
    turn = 1 - 2 * core

    def chip_at(offset):
        return (chip + offset + chips) % chips

    fwd = 2 * chip_at(turn) + core
    bwd = 2 * chip_at(-turn) + core

    barrier = pltpu.get_barrier_semaphore()
    for j in range(1, tp_size):
        pl.semaphore_signal(barrier, inc=1, device_id={"tp": (me + j) % tp_size}, device_id_type=MESH_ID)
    for j in range(1, vp_size):
        pl.semaphore_signal(barrier, inc=1, device_id={"vp": (my_vp + j) % vp_size}, device_id_type=MESH_ID)

    def block_of(phase, half, sign):
        if phase == 0:
            return chip_at(2)
        if phase == 3:
            return chip
        if (phase == 1) == (half == 0):
            return chip_at(-sign)
        return chip_at(sign)

    def first_row(phase, half, own):
        if own:
            return (2 * block_of(phase, half, turn) + core) * own_cols + half * half_cols
        return (2 * block_of(phase, half, -turn) + 1 - core) * own_cols + half * half_cols

    def table_load(phase, half, own):
        count = half_cols if half == 0 else own_cols - half_cols
        span = pl.ds(pl.multiple_of(first_row(phase, half, own), 16), count)
        return pltpu.make_async_copy(emb.at[span], e_all.at[span], e_sem.at[phase * 4 + half * 2 + own])

    for phase in range(4):
        for own in range(2):
            for half in range(2):
                table_load(phase, half, own).start()

    def stat_copy(s, j):
        return pltpu.make_async_remote_copy(
            src_ref=stat_src.at[s], dst_ref=stat_in.at[s, j - 1],
            send_sem=stat_send.at[s, j - 1], recv_sem=stat_recv.at[s, j - 1],
            device_id={"tp": (me + j) % tp_size}, device_id_type=MESH_ID)

    def vp_copy(src, dst, send, recv, j):
        return pltpu.make_async_remote_copy(
            src_ref=src, dst_ref=dst.at[j - 1], send_sem=send.at[j - 1], recv_sem=recv.at[j - 1],
            device_id={"vp": (my_vp + j) % vp_size}, device_id_type=MESH_ID)

    def stat_total(s):
        total = stat_src[s]
        for j in range(1, tp_size):
            stat_copy(s, j).wait()
            total = total + stat_in[s, j - 1]
        return total[:1]

    x = hid[...].astype(jnp.float32)
    stat_src[0] = jnp.broadcast_to(_row_stats(x), (8, LANES))
    pl.semaphore_wait(barrier, tp_size - 1 + vp_size - 1)
    for j in range(1, tp_size):
        stat_copy(0, j).start()
    xn[...] = _normalize(x, stat_total(0), g1[...], b1[...], full_width)

    def chunk_dot(dst, row0, cols):
        for c in range(0, cols, DOT_COLS):
            n = min(DOT_COLS, cols - c)
            part = e_all[pl.ds(pl.multiple_of(row0 + c, 16), n), :]
            dst[:, c : c + n] = lax.dot_general(
                xn[...], part, (((1,), (1,)), ((), ())), preferred_element_type=jnp.float32)
        if cols % LANES:
            end = pl.cdiv(cols, LANES) * LANES
            dst[:, cols:end] = jnp.zeros((rows, end - cols), jnp.float32)

    def cols_of(half, last):
        return (tail, tail_pad) if half == 1 and last else (CHUNK, CHUNK)

    def peer_copy(phase, half, k, last):
        lanes = pl.ds(0, cols_of(half, last)[1])
        slot, at = half * half_chunks + k, phase * n_chunks + half * half_chunks + k
        return pltpu.make_async_remote_copy(
            src_ref=to_peer.at[slot, :, lanes], dst_ref=from_peer.at[at, :, lanes],
            send_sem=peer_send.at[slot], recv_sem=peer_recv.at[at],
            device_id={"tp": peer}, device_id_type=MESH_ID)

    def ring_copy(phase, half, k, last):
        lanes = pl.ds(0, cols_of(half, last)[1])
        at = phase * n_chunks + half * half_chunks + k
        forward = (half == 0) != (phase == 1)
        return pltpu.make_async_remote_copy(
            src_ref=mine.at[at, :, lanes], dst_ref=ring.at[at, :, lanes],
            send_sem=ring_send.at[at], recv_sem=ring_recv.at[at],
            device_id={"tp": fwd if forward else bwd}, device_id_type=MESH_ID)

    def at_of(phase, half, k):
        return phase * n_chunks + half * half_chunks + k

    def add_into(at, others, width_):
        for r in range(0, rows, 8):
            v = mine[at, r : r + 8, :width_]
            for ref, i in others:
                v = v + ref[i, r : r + 8, :width_]
            mine[at, r : r + 8, :width_] = v

    def product(phase, k, last):
        for half in range(2):
            if phase:
                peer_copy(phase - 1, half, k, last).wait_send()
            chunk_dot(to_peer.at[half * half_chunks + k], first_row(phase, half, 0) + k * CHUNK, cols_of(half, last)[0])
        for half in range(2):
            peer_copy(phase, half, k, last).start()
        for half in range(2):
            chunk_dot(mine.at[at_of(phase, half, k)], first_row(phase, half, 1) + k * CHUNK, cols_of(half, last)[0])
        if phase < 2:
            for half in range(2):
                at = at_of(phase, half, k)
                peer_copy(phase, half, k, last).wait_recv()
                add_into(at, [(from_peer, at)], cols_of(half, last)[1])
            for half in range(2):
                ring_copy(phase, half, k, last).start()

    def each_chunk(body):
        def step(k, carry):
            body(k, False)
            return carry

        lax.fori_loop(0, half_chunks - 1, step, 0)
        body(half_chunks - 1, True)

    def wait_table(phase):
        for own in range(2):
            for half in range(2):
                table_load(phase, half, own).wait()

    wait_table(0)
    each_chunk(functools.partial(product, 0))

    for phase in range(1, 4):
        wait_table(phase)

    def pick_rows():
        wanted = tok[...].astype(jnp.float32) - (my_vp * vocab_rows).astype(jnp.float32)
        wanted = jnp.concatenate([wanted, jnp.zeros((1, LANES - rows), jnp.float32)], axis=1)
        wanted = _as_columns(wanted)[:rows].astype(jnp.int32)
        lane = lax.broadcasted_iota(jnp.int32, wanted.shape, 1)

        def add(first, count):
            hits = []
            for c in range(0, count, LANES):
                hits.append(jnp.where(lane + (first + c) == wanted, 1.0, 0.0).astype(jnp.bfloat16))
            e_src[...] += jnp.dot(
                jnp.concatenate(hits, axis=1), e_all[pl.ds(pl.multiple_of(first, LANES), count), :],
                preferred_element_type=jnp.float32)

        def step(i, carry):
            add(i * PICK, PICK)
            return carry

        e_src[...] = jnp.zeros_like(e_src)
        lax.fori_loop(0, vocab_rows // PICK, step, 0)
        if vocab_rows % PICK:
            add(vocab_rows // PICK * PICK, vocab_rows % PICK)

    each_chunk(functools.partial(product, 1))
    pick_rows()
    for j in range(1, vp_size):
        vp_copy(e_src, e_in, row_send, row_recv, j).start()
    each_chunk(functools.partial(product, 2))
    e_row = e_src[...]
    for j in range(1, vp_size):
        vp_copy(e_src, e_in, row_send, row_recv, j).wait()
        e_row = e_row + e_in[j - 1]
    stat_src[1] = jnp.broadcast_to(_row_stats(e_row), (8, LANES))
    for j in range(1, tp_size):
        stat_copy(1, j).start()

    def forward_chunk(k, last):
        for half in range(2):
            at = at_of(2, half, k)
            peer_copy(2, half, k, last).wait_recv()
            ring_copy(0, half, k, last).wait_recv()
            add_into(at, [(from_peer, at), (ring, at_of(0, half, k))], cols_of(half, last)[1])
        for half in range(2):
            ring_copy(2, half, k, last).start()

    each_chunk(forward_chunk)
    each_chunk(functools.partial(product, 3))

    e_row = e_src[...]
    for j in range(1, vp_size):
        e_row = e_row + e_in[j - 1]
    nin_out[...] = _normalize(e_row, stat_total(1), g2[...], b2[...], full_width)

    top[...] = jnp.full(top.shape, jnp.finfo(jnp.float32).min, jnp.float32)
    acc[...] = jnp.zeros_like(acc)

    def z_copy(half, k, last):
        n = cols_of(half, last)[1]
        off = pl.multiple_of((half * half_chunks + k) * CHUNK, LANES)
        return pltpu.make_async_copy(
            mine.at[at_of(3, half, k), :, pl.ds(0, n)], z_out.at[:, pl.ds(off, n)],
            z_sem.at[half * half_chunks + k])

    def finish_chunk(k, last):
        for half in range(2):
            at = at_of(3, half, k)
            real, padded = cols_of(half, last)
            peer_copy(3, half, k, last).wait_recv()
            ring_copy(1, half, k, last).wait_recv()
            ring_copy(2, half, k, last).wait_recv()
            for r in range(0, rows, 8):
                group = slice(r, r + 8)
                tiles = []
                for c in range(0, padded, LANES):
                    lane = slice(c, c + LANES)
                    v = (mine[at, group, lane] + from_peer[at, group, lane]) + (
                        ring[at_of(1, half, k), group, lane] + ring[at_of(2, half, k), group, lane])
                    mine[at, group, lane] = v
                    if c + LANES > real:
                        v = jnp.where(lax.broadcasted_iota(jnp.int32, v.shape, 1) < real - c, v, -jnp.inf)
                    tiles.append(v)
                best = top[group, :]
                old = best
                for v in tiles:
                    best = jnp.maximum(best, v)
                total = acc[group, :] * jnp.exp(old - best)
                for v in tiles:
                    total = total + jnp.exp(v - best)
                top[group, :] = best
                acc[group, :] = total
        for half in range(2):
            z_copy(half, k, last).start()

    each_chunk(finish_chunk)

    tops = jnp.concatenate([top[...], top[...]], axis=0).T
    sums = jnp.concatenate([acc[...], acc[...]], axis=0).T
    best = jnp.max(tops, axis=0, keepdims=True)
    total = jnp.sum(sums * jnp.exp(tops - best), axis=0, keepdims=True)

    def merge(items):
        new = functools.reduce(jnp.maximum, [b for b, _ in items])
        return new, functools.reduce(jnp.add, [t * jnp.exp(b - new) for b, t in items])

    stat_src[2, 0:1, :] = best
    stat_src[2, 1:2, :] = total
    for j in range(1, tp_size):
        stat_copy(2, j).start()
    items = [(best, total)]
    for j in range(1, tp_size):
        stat_copy(2, j).wait()
        items.append((stat_in[2, j - 1, 0:1, :], stat_in[2, j - 1, 1:2, :]))
    best, total = merge(items)
    v_src[0:1, :] = best
    v_src[1:2, :] = total
    for j in range(1, vp_size):
        vp_copy(v_src, v_in, v_send, v_recv, j).start()
    items = [(best, total)]
    for j in range(1, vp_size):
        vp_copy(v_src, v_in, v_send, v_recv, j).wait()
        items.append((v_in[j - 1, 0:1, :], v_in[j - 1, 1:2, :]))
    best, total = merge(items)
    ls_out[...] = jnp.broadcast_to(best + jnp.log(total), ls_out.shape)

    def drain(k, last):
        for half in range(2):
            z_copy(half, k, last).wait()
            peer_copy(3, half, k, last).wait_send()
            for phase in range(3):
                ring_copy(phase, half, k, last).wait_send()

    each_chunk(drain)


def _subtract_kernel(z, ls, nin, logprobs, log_sum, next_in):
    rows = logprobs.shape[0]
    cols = _as_columns(ls[0:1, :])[:rows]
    n = logprobs.shape[1]
    for c in range(0, n, LANES):
        w = min(LANES, n - c)
        logprobs[:, c : c + w] = z[:, c : c + w] - cols[:, :w]
    log_sum[...] = ls[0:1, :rows]
    next_in[...] = nin[...]


def solution(mesh):
    tp_size = mesh.shape["tp"]
    vp_size = mesh.shape["vp"]

    def per_device(hidden, lnf_gain, lnf_bias, emb_table, next_tok, eln_gain, eln_bias):
        rows, width = hidden.shape
        own_cols = emb_table.shape[0] // tp_size
        n_chunks = pl.cdiv(own_cols, CHUNK)
        padded = pl.cdiv(own_cols, LANES) * LANES
        f32 = jnp.float32
        vmem = pl.BlockSpec(memory_space=pltpu.VMEM)
        dma = pltpu.SemaphoreType.DMA
        z, ls, nin = pl.pallas_call(
            functools.partial(_head_kernel, tp_size, vp_size),
            out_shape=(
                jax.ShapeDtypeStruct((rows, padded), f32),
                jax.ShapeDtypeStruct((8, LANES), f32),
                jax.ShapeDtypeStruct((rows, width), jnp.bfloat16),
            ),
            in_specs=[vmem] * 6 + [pl.BlockSpec(memory_space=pl.ANY)],
            out_specs=(pl.BlockSpec(memory_space=pl.ANY), vmem, vmem),
            scratch_shapes=[
                pltpu.VMEM(emb_table.shape, emb_table.dtype),
                pltpu.VMEM((4 * n_chunks, rows, CHUNK), f32),
                pltpu.VMEM((4 * n_chunks, rows, CHUNK), f32),
                pltpu.VMEM((n_chunks, rows, CHUNK), f32),
                pltpu.VMEM((3 * n_chunks, rows, CHUNK), f32),
                pltpu.VMEM((rows, width), jnp.bfloat16),
                pltpu.VMEM((rows, LANES), f32),
                pltpu.VMEM((rows, LANES), f32),
                pltpu.VMEM((rows, width), f32),
                pltpu.VMEM((vp_size - 1, rows, width), f32),
                pltpu.VMEM((3, 8, LANES), f32),
                pltpu.VMEM((3, tp_size - 1, 8, LANES), f32),
                pltpu.VMEM((8, LANES), f32),
                pltpu.VMEM((vp_size - 1, 8, LANES), f32),
                dma((16,)),
                dma((n_chunks,)),
                dma((4 * n_chunks,)),
                dma((3 * n_chunks,)),
                dma((3 * n_chunks,)),
                dma((3, tp_size - 1)),
                dma((3, tp_size - 1)),
                dma((vp_size - 1,)),
                dma((vp_size - 1,)),
                dma((vp_size - 1,)),
                dma((vp_size - 1,)),
                dma((n_chunks,)),
            ],
            compiler_params=pltpu.CompilerParams(
                collective_id=0, has_side_effects=True, vmem_limit_bytes=63_000_000),
            name="vocab_head",
        )(
            hidden, lnf_gain.reshape(1, width), lnf_bias.reshape(1, width),
            eln_gain.reshape(1, width), eln_bias.reshape(1, width), next_tok.reshape(1, rows), emb_table,
        )
        logprobs, log_sum, next_in = pl.pallas_call(
            _subtract_kernel,
            out_shape=(
                jax.ShapeDtypeStruct((rows, own_cols), f32),
                jax.ShapeDtypeStruct((1, rows), f32),
                jax.ShapeDtypeStruct((rows, width), jnp.bfloat16),
            ),
            in_specs=[vmem] * 3,
            out_specs=(vmem,) * 3,
            name="log_probs",
        )(z, ls, nin)
        return logprobs, log_sum.reshape(rows), next_in

    return jax.shard_map(
        per_device,
        mesh=mesh,
        in_specs=(P("dp", "tp"), P("tp"), P("tp"), P("vp", "tp"), P("dp"), P("tp"), P("tp")),
        out_specs=(P("dp", ("vp", "tp")), P("dp"), P("dp", "tp")),
        check_vma=False,
    )
```

```python
import functools

import jax
import jax.numpy as jnp
from jax import lax
from jax.experimental import pallas as pl
from jax.experimental.pallas import tpu as pltpu
from jax.sharding import PartitionSpec as P

NORM_EPS = 1e-5
LANES = 128
CHUNK = 1024
HEAD = 256
DOT_COLS = 512
PICK = 1280
MESH_ID = pl.DeviceIdType.MESH


def _row_stats(x):
    sums = x[:, :LANES]
    squares = sums * sums
    for c in range(LANES, x.shape[1], LANES):
        part = x[:, c : c + LANES]
        sums = sums + part
        squares = squares + part * part
    both = jnp.concatenate([sums, squares], axis=0)
    return jnp.sum(both.T, axis=0, keepdims=True)


def _as_columns(row):
    return jnp.broadcast_to(row, (LANES, LANES)).T


def _normalize(x, total, gain, bias, full_width):
    rows = x.shape[0]
    cols = _as_columns(total)
    mean = cols[:rows] / full_width
    var = cols[rows : 2 * rows] / full_width - mean * mean
    rstd = lax.rsqrt(var + NORM_EPS)
    parts = []
    for c in range(0, x.shape[1], LANES):
        scaled = (x[:, c : c + LANES] - mean) * rstd
        parts.append(scaled * gain[:, c : c + LANES] + bias[:, c : c + LANES])
    return jnp.concatenate(parts, axis=1).astype(jnp.bfloat16)


def _unpacked(packed, first_row, rows_per_group, cols):
    group, r = first_row // rows_per_group, first_row % rows_per_group
    v = packed[r : r + 8, :]
    return pltpu.roll(v, LANES - group * cols, 1) if group else v


def _head_kernel(
    tp_size, vp_size,
    hid_hbm, g1_hbm, b1_hbm, g2_hbm, b2_hbm, tok_hbm, emb,
    z_out, ls_out, nin_out,
    hid, norms, tok,
    e_all, mine, from_peer, to_peer, ring, xn,
    top, acc, e_src, e_in, stat_src, stat_in, lse_src, lse_tp, lse_vp,
    small_sem, e_sem, peer_send, peer_recv, ring_send, ring_recv, head_send, head_recv,
    stat_send, stat_recv, row_sem, lse_sem,
):
    rows, width = hid.shape
    full_width = width * tp_size
    vocab_rows = emb.shape[0]
    own_cols = vocab_rows // tp_size
    chips = tp_size // 2
    n_chunks = pl.cdiv(own_cols, CHUNK)
    half_chunks = n_chunks // 2
    half_cols = half_chunks * CHUNK
    tail = own_cols - (n_chunks - 1) * CHUNK
    rest = tail % LANES
    rest_rows = rows * rest // LANES

    def buffer_rows(cols):
        return cols // LANES * rows + (rest_rows if cols % LANES else 0)

    me = lax.axis_index("tp")
    my_vp = lax.axis_index("vp")
    chip = me // 2
    core = me % 2
    peer = 2 * chip + 1 - core
    turn = 1 - 2 * core

    def chip_at(offset):
        return (chip + offset + chips) % chips

    fwd = 2 * chip_at(turn) + core
    bwd = 2 * chip_at(-turn) + core

    barrier = pltpu.get_barrier_semaphore()
    far_first = sorted(range(1, tp_size), key=lambda j: -min(j, tp_size - j))
    for j in far_first:
        pl.semaphore_signal(barrier, inc=1, device_id={"tp": (me + j) % tp_size}, device_id_type=MESH_ID)
    for j in range(1, vp_size):
        pl.semaphore_signal(barrier, inc=1, device_id={"vp": (my_vp + j) % vp_size}, device_id_type=MESH_ID)

    hid_load = pltpu.make_async_copy(hid_hbm, hid, small_sem.at[0])
    tok_load = pltpu.make_async_copy(tok_hbm, tok, small_sem.at[1])
    hid_load.start()
    for i, src in enumerate([g1_hbm, b1_hbm, g2_hbm, b2_hbm]):
        pltpu.make_async_copy(src, norms.at[i], small_sem.at[2]).start()
    tok_load.start()

    def block_of(phase, half, sign):
        if phase == 0:
            return chip_at(2)
        if phase == 3:
            return chip
        if (phase == 1) == (half == 0):
            return chip_at(-sign)
        return chip_at(sign)

    def first_row(phase, half, own):
        if own:
            return (2 * block_of(phase, half, turn) + core) * own_cols + half * half_cols
        return (2 * block_of(phase, half, -turn) + 1 - core) * own_cols + half * half_cols

    def table_load(phase, half, own):
        count = half_cols if half == 0 else own_cols - half_cols
        span = pl.ds(pl.multiple_of(first_row(phase, half, own), 16), count)
        return pltpu.make_async_copy(emb.at[span], e_all.at[span], e_sem.at[phase])

    def wait_table(phase):
        span = pl.ds(0, 2 * own_cols)
        pltpu.make_async_copy(emb.at[span], e_all.at[span], e_sem.at[phase]).wait()

    hid_load.wait()
    pltpu.make_async_copy(norms, norms, small_sem.at[2]).wait()
    tok_load.wait()
    for phase in range(4):
        for own in range(2):
            for half in range(2):
                table_load(phase, half, own).start()

    def share(src, dst, send, recv, axis, j):
        size, at = (tp_size, me) if axis == "tp" else (vp_size, my_vp)
        return pltpu.make_async_remote_copy(
            src_ref=src, dst_ref=dst.at[j - 1], send_sem=send, recv_sem=recv,
            device_id={axis: (at + j) % size}, device_id_type=MESH_ID)

    def all_shared(dst, send, recv, axis):
        at = (me + 1) % tp_size if axis == "tp" else (my_vp + 1) % vp_size
        return pltpu.make_async_remote_copy(
            src_ref=dst, dst_ref=dst, send_sem=send, recv_sem=recv,
            device_id={axis: at}, device_id_type=MESH_ID)

    def share_stats(s):
        for j in far_first:
            share(stat_src.at[s], stat_in.at[s], stat_send.at[s], stat_recv.at[s], "tp", j).start()

    def stat_total(s):
        all_shared(stat_in.at[s], stat_send.at[s], stat_recv.at[s], "tp").wait_recv()
        total = stat_src[s]
        for j in range(1, tp_size):
            total = total + stat_in[s, j - 1]
        return total

    x = hid[...].astype(jnp.float32)
    stat_src[0] = _row_stats(x)
    pl.semaphore_wait(barrier, tp_size - 1 + vp_size - 1)
    share_stats(0)
    xn[...] = _normalize(x, stat_total(0), norms[0], norms[1], full_width)

    def chunk_dot(dst, base, row0, first, cols):
        for c in range(first, cols, DOT_COLS):
            n = min(DOT_COLS, cols - c)
            part = e_all[pl.ds(pl.multiple_of(row0 + c, 16), n), :]
            v = lax.dot_general(xn[...], part, (((1,), (1,)), ((), ())), preferred_element_type=jnp.float32)
            for t in range(0, n, LANES):
                at = base + (c + t) // LANES * rows
                if t + LANES <= n:
                    dst[pl.ds(at, rows), :] = v[:, t : t + LANES]
                else:
                    dst[pl.ds(at, rest_rows), :] = jnp.concatenate(
                        [v[q : q + rest_rows, t:n] for q in range(0, rows, rest_rows)], axis=1)

    def cols_of(half, last):
        return tail if half == 1 and last else CHUNK

    def at_of(phase, half, k):
        return phase * n_chunks + half * half_chunks + k

    own_rows = buffer_rows(own_cols)

    def base_of(phase, half, k):
        return pl.multiple_of(phase * own_rows + (half * half_chunks + k) * buffer_rows(CHUNK), 8)

    def span_of(phase, half, k, last):
        begin = buffer_rows(HEAD) if phase == 0 and isinstance(k, int) and k == 0 else 0
        return pl.ds(base_of(phase, half, k) + begin, buffer_rows(cols_of(half, last)) - begin)

    def peer_sems(phase, half, k):
        slot = half * half_chunks + k
        return peer_send.at[slot], peer_recv.at[phase * n_chunks + slot if phase < 2 else 2 * n_chunks + phase - 2]

    def peer_copy(phase, half, k, last):
        into = span_of(phase, half, k, last)
        begin = into.start - base_of(phase, half, k)
        slot = half * half_chunks + k
        send, recv = peer_sems(phase, half, k)
        return pltpu.make_async_remote_copy(
            src_ref=to_peer.at[slot, pl.ds(begin, into.size)], dst_ref=from_peer.at[into],
            send_sem=send, recv_sem=recv, device_id={"tp": peer}, device_id_type=MESH_ID)

    def ring_recv_of(phase, half, k):
        return ring_recv.at[phase if phase < 2 else 2 + half * half_chunks + k]

    def ring_copy(phase, half, k, last):
        span = span_of(phase, half, k, last)
        forward = (half == 0) != (phase == 1)
        return pltpu.make_async_remote_copy(
            src_ref=mine.at[span], dst_ref=ring.at[span],
            send_sem=ring_send.at[0], recv_sem=ring_recv_of(phase, half, k),
            device_id={"tp": fwd if forward else bwd}, device_id_type=MESH_ID)

    def whole_phase(ref, phase):
        return ref.at[pl.ds(phase * own_rows, own_rows)]

    def wait_peer_phase(phase):
        ref = whole_phase(from_peer, phase)
        pltpu.make_async_remote_copy(
            src_ref=ref, dst_ref=ref, send_sem=peer_send.at[0], recv_sem=peer_sems(phase, 0, 0)[1],
            device_id={"tp": peer}, device_id_type=MESH_ID).wait_recv()

    def wait_ring_phase(phase):
        ref = whole_phase(ring, phase)
        pltpu.make_async_remote_copy(
            src_ref=ref, dst_ref=ref, send_sem=ring_send.at[0], recv_sem=ring_recv.at[phase],
            device_id={"tp": fwd}, device_id_type=MESH_ID).wait_recv()

    head_rows = pl.ds(0, buffer_rows(HEAD))

    def head_peer_copy(half):
        slot = half * half_chunks
        return pltpu.make_async_remote_copy(
            src_ref=to_peer.at[slot, head_rows], dst_ref=from_peer.at[pl.ds(slot * buffer_rows(CHUNK), head_rows.size)],
            send_sem=head_send.at[half], recv_sem=head_recv.at[half],
            device_id={"tp": peer}, device_id_type=MESH_ID)

    def head_ring_copy(half):
        span = pl.ds(half * half_chunks * buffer_rows(CHUNK), head_rows.size)
        return pltpu.make_async_remote_copy(
            src_ref=mine.at[span], dst_ref=ring.at[span],
            send_sem=ring_send.at[0], recv_sem=ring_recv.at[0],
            device_id={"tp": bwd if half else fwd}, device_id_type=MESH_ID)

    def add_into(base, others, begin, end):
        for r in range(begin, end, 8):
            v = mine[pl.ds(base + r, 8), :]
            for ref, at in others:
                v = v + ref[pl.ds(at + r, 8), :]
            mine[pl.ds(base + r, 8), :] = v

    def to_peer_dot(phase, half, k, last, first=0, end=None):
        chunk_dot(to_peer.at[half * half_chunks + k], 0, first_row(phase, half, 0) + k * CHUNK,
                  first, end or cols_of(half, last))

    def mine_dot(phase, half, k, last, first=0, end=None):
        if phase < 3:
            dst, base = mine, base_of(phase, half, k)
        else:
            dst, base = z_out, base_of(0, half, k)
        chunk_dot(dst, base, first_row(phase, half, 1) + k * CHUNK, first, end or cols_of(half, last))

    def first_product():
        for half in range(2):
            to_peer_dot(0, half, 0, False, 0, HEAD)
        for half in range(2):
            head_peer_copy(half).start()
        for half in range(2):
            mine_dot(0, half, 0, False, 0, HEAD)
        for half in range(2):
            to_peer_dot(0, half, 0, False, HEAD)
        for half in range(2):
            peer_copy(0, half, 0, False).start()
        for half in range(2):
            at = base_of(0, half, 0)
            head_peer_copy(half).wait_recv()
            add_into(at, [(from_peer, at)], 0, buffer_rows(HEAD))
        for half in range(2):
            head_ring_copy(half).start()
        for half in range(2):
            mine_dot(0, half, 0, False, HEAD)
        for half in range(2):
            at = base_of(0, half, 0)
            peer_copy(0, half, 0, False).wait_recv()
            add_into(at, [(from_peer, at)], buffer_rows(HEAD), buffer_rows(CHUNK))
        for half in range(2):
            ring_copy(0, half, 0, False).start()
        for half in range(2):
            head_peer_copy(half).wait_send()

    def product(phase, k, last):
        for half in range(2):
            if phase:
                peer_copy(phase - 1, half, k, last).wait_send()
            to_peer_dot(phase, half, k, last)
        for half in range(2):
            peer_copy(phase, half, k, last).start()
        for half in range(2):
            mine_dot(phase, half, k, last)
        if phase < 2:
            for half in range(2):
                at = base_of(phase, half, k)
                peer_copy(phase, half, k, last).wait_recv()
                add_into(at, [(from_peer, at)], 0, buffer_rows(cols_of(half, last)))
            for half in range(2):
                ring_copy(phase, half, k, last).start()

    def each_chunk(body, begin=0):
        def step(k, carry):
            body(k, False)
            return carry

        for k in range(begin, 1):
            body(k, False)
        lax.fori_loop(1, half_chunks - 1, step, 0)
        body(half_chunks - 1, True)

    wait_table(0)
    first_product()
    each_chunk(functools.partial(product, 0), 1)

    for phase in range(1, 4):
        wait_table(phase)

    def pick_rows():
        wanted = tok[...].astype(jnp.float32) - (my_vp * vocab_rows).astype(jnp.float32)
        wanted = jnp.concatenate([wanted, jnp.zeros((1, LANES - rows), jnp.float32)], axis=1)
        wanted = _as_columns(wanted)[:rows].astype(jnp.int32)
        lane = lax.broadcasted_iota(jnp.int32, wanted.shape, 1)

        def add(first, count):
            hits = []
            for c in range(0, count, LANES):
                hits.append(jnp.where(lane + (first + c) == wanted, 1.0, 0.0).astype(jnp.bfloat16))
            e_src[...] += jnp.dot(
                jnp.concatenate(hits, axis=1), e_all[pl.ds(pl.multiple_of(first, LANES), count), :],
                preferred_element_type=jnp.float32)

        def step(i, carry):
            add(i * PICK, PICK)
            return carry

        e_src[...] = jnp.zeros_like(e_src)
        lax.fori_loop(0, vocab_rows // PICK, step, 0)
        if vocab_rows % PICK:
            add(vocab_rows // PICK * PICK, vocab_rows % PICK)

    each_chunk(functools.partial(product, 1))
    pick_rows()
    for j in range(1, vp_size):
        share(e_src, e_in, row_sem.at[0], row_sem.at[1], "vp", j).start()
    each_chunk(functools.partial(product, 2))

    def token_rows():
        rows_sum = e_src[...]
        for j in range(1, vp_size):
            rows_sum = rows_sum + e_in[j - 1]
        return rows_sum

    all_shared(e_in, row_sem.at[0], row_sem.at[1], "vp").wait()
    stat_src[1] = _row_stats(token_rows())
    share_stats(1)

    def forward_chunk(k, last):
        for half in range(2):
            at = base_of(2, half, k)
            add_into(at, [(from_peer, at), (ring, base_of(0, half, k))], 0, buffer_rows(cols_of(half, last)))
        for half in range(2):
            ring_copy(2, half, k, last).start()

    wait_peer_phase(2)
    wait_ring_phase(0)
    each_chunk(forward_chunk)
    each_chunk(functools.partial(product, 3))
    nin_out[...] = _normalize(token_rows(), stat_total(1), norms[2], norms[3], full_width)

    top[...] = jnp.full(top.shape, jnp.finfo(jnp.float32).min, jnp.float32)
    acc[...] = jnp.zeros_like(acc)

    def finish_chunk(k, last):
        for half in range(2):
            cols = cols_of(half, last)
            base, peer_base = base_of(0, half, k), base_of(3, half, k)
            single, chain = base_of(1, half, k), base_of(2, half, k)
            ring_copy(2, half, k, last).wait_recv()

            def final(r):
                v = (z_out[pl.ds(base + r, 8), :] + from_peer[pl.ds(peer_base + r, 8), :]) + (
                    ring[pl.ds(single + r, 8), :] + ring[pl.ds(chain + r, 8), :])
                z_out[pl.ds(base + r, 8), :] = v
                return v

            full = cols // LANES
            if cols % LANES:
                packed = jnp.concatenate([final(full * rows + r) for r in range(0, rest_rows, 8)], axis=0)
            for r in range(0, rows, 8):
                tiles = [final(t * rows + r) for t in range(full)]
                if cols % LANES:
                    v = _unpacked(packed, r, rest_rows, rest)
                    tiles.append(jnp.where(lax.broadcasted_iota(jnp.int32, v.shape, 1) < rest, v, -jnp.inf))
                old = top[r : r + 8, :]
                best = functools.reduce(jnp.maximum, tiles, old)
                total = acc[r : r + 8, :] * jnp.exp(old - best)
                for v in tiles:
                    total = total + jnp.exp(v - best)
                top[r : r + 8, :] = best
                acc[r : r + 8, :] = total

    wait_peer_phase(3)
    wait_ring_phase(1)
    each_chunk(finish_chunk)

    tops = jnp.concatenate([top[...], top[...]], axis=0).T
    sums = jnp.concatenate([acc[...], acc[...]], axis=0).T
    best = jnp.max(tops, axis=0, keepdims=True)
    total = jnp.sum(sums * jnp.exp(tops - best), axis=0, keepdims=True)

    def merge(best, total, other):
        tops = [best] + [other[j, 0:1, :] for j in range(other.shape[0])]
        sums = [total] + [other[j, 1:2, :] for j in range(other.shape[0])]
        new = functools.reduce(jnp.maximum, tops)
        return new, functools.reduce(jnp.add, [t * jnp.exp(b - new) for b, t in zip(tops, sums)])

    stages = (("tp", far_first, lse_tp), ("vp", range(1, vp_size), lse_vp))
    for i, (axis, order, other) in enumerate(stages):
        lse_src[i, 0:1, :] = best
        lse_src[i, 1:2, :] = total
        for j in order:
            share(lse_src.at[i], other, lse_sem.at[2 * i], lse_sem.at[2 * i + 1], axis, j).start()
        all_shared(other, lse_sem.at[2 * i], lse_sem.at[2 * i + 1], axis).wait_recv()
        best, total = merge(best, total, other)
    ls_out[...] = jnp.broadcast_to(best + jnp.log(total), ls_out.shape)

    for s in range(2):
        all_shared(stat_in.at[s], stat_send.at[s], stat_recv.at[s], "tp").wait_send()
    for i, (axis, _, other) in enumerate(stages):
        all_shared(other, lse_sem.at[2 * i], lse_sem.at[2 * i + 1], axis).wait_send()
    pltpu.make_async_remote_copy(
        src_ref=mine, dst_ref=ring, send_sem=ring_send.at[0], recv_sem=ring_recv.at[0],
        device_id={"tp": fwd}, device_id_type=MESH_ID).wait_send()
    each_chunk(lambda k, last: [peer_copy(3, half, k, last).wait_send() for half in range(2)])


def _subtract_kernel(z, ls, nin, logprobs, log_sum, next_in, out, sums, sems):
    rows, n = out.shape
    rest = n % LANES
    rest_rows = rows * rest // LANES
    step = rows // 4
    copies = [
        pltpu.make_async_copy(nin, next_in, sems.at[4]),
        pltpu.make_async_copy(sums, log_sum, sems.at[5]),
    ]
    copies[0].start()
    sums[...] = ls[0:1, :rows]
    cols = _as_columns(ls[0:1, :])[:rows]
    packed = z[n // LANES * rows :, :]
    for i in range(4):
        for r in range(i * step, (i + 1) * step, 8):
            for t in range(n // LANES):
                out[r : r + 8, t * LANES : (t + 1) * LANES] = z[t * rows + r : t * rows + r + 8, :] - cols[r : r + 8]
            if rest:
                v = _unpacked(packed, r, rest_rows, rest) - cols[r : r + 8]
                out[r : r + 8, n - rest :] = v[:, :rest]
        span = pl.ds(i * step, step)
        copies.append(pltpu.make_async_copy(out.at[span], logprobs.at[span], sems.at[i]))
        copies[-1].start()
        if i == 0:
            copies[1].start()
    for copy in copies:
        copy.wait()


def solution(mesh):
    tp_size = mesh.shape["tp"]
    vp_size = mesh.shape["vp"]

    def per_device(hidden, lnf_gain, lnf_bias, emb_table, next_tok, eln_gain, eln_bias):
        rows, width = hidden.shape
        own_cols = emb_table.shape[0] // tp_size
        n_chunks = pl.cdiv(own_cols, CHUNK)
        f32 = jnp.float32
        vmem = pl.BlockSpec(memory_space=pltpu.VMEM)
        hbm = pl.BlockSpec(memory_space=pltpu.HBM)
        dma = pltpu.SemaphoreType.DMA
        own_rows = rows * own_cols // LANES
        z, ls, nin = pl.pallas_call(
            functools.partial(_head_kernel, tp_size, vp_size),
            out_shape=(
                pltpu.VMEM((own_rows, LANES), f32),
                pltpu.VMEM((8, LANES), f32),
                pltpu.VMEM((rows, width), jnp.bfloat16),
            ),
            in_specs=[hbm] * 7,
            out_specs=(vmem,) * 3,
            scratch_shapes=[
                pltpu.VMEM((rows, width), hidden.dtype),
                pltpu.VMEM((4, 1, width), f32),
                pltpu.VMEM((1, rows), jnp.int32),
                pltpu.VMEM(emb_table.shape, emb_table.dtype),
                pltpu.VMEM((3 * own_rows, LANES), f32),
                pltpu.VMEM((4 * own_rows, LANES), f32),
                pltpu.VMEM((n_chunks, rows * CHUNK // LANES, LANES), f32),
                pltpu.VMEM((3 * own_rows, LANES), f32),
                pltpu.VMEM((rows, width), jnp.bfloat16),
                pltpu.VMEM((rows, LANES), f32),
                pltpu.VMEM((rows, LANES), f32),
                pltpu.VMEM((rows, width), f32),
                pltpu.VMEM((vp_size - 1, rows, width), f32),
                pltpu.VMEM((2, 1, LANES), f32),
                pltpu.VMEM((2, tp_size - 1, 1, LANES), f32),
                pltpu.VMEM((2, 2, LANES), f32),
                pltpu.VMEM((tp_size - 1, 2, LANES), f32),
                pltpu.VMEM((vp_size - 1, 2, LANES), f32),
                dma((3,)),
                dma((4,)),
                dma((n_chunks,)),
                dma((2 * n_chunks + 2,)),
                dma((1,)),
                dma((2 + n_chunks,)),
                dma((2,)),
                dma((2,)),
                dma((2,)),
                dma((2,)),
                dma((2,)),
                dma((4,)),
            ],
            compiler_params=pltpu.CompilerParams(
                collective_id=0, has_side_effects=True, vmem_limit_bytes=58_000_000),
            name="vocab_head",
        )(
            hidden, lnf_gain.reshape(1, width), lnf_bias.reshape(1, width),
            eln_gain.reshape(1, width), eln_bias.reshape(1, width), next_tok.reshape(1, rows), emb_table,
        )
        logprobs, log_sum, next_in = pl.pallas_call(
            _subtract_kernel,
            out_shape=(
                jax.ShapeDtypeStruct((rows, own_cols), f32),
                jax.ShapeDtypeStruct((1, rows), f32),
                jax.ShapeDtypeStruct((rows, width), jnp.bfloat16),
            ),
            in_specs=[vmem] * 3,
            out_specs=(hbm,) * 3,
            scratch_shapes=[pltpu.VMEM((rows, own_cols), f32), pltpu.VMEM((1, rows), f32), dma((6,))],
            compiler_params=pltpu.CompilerParams(vmem_limit_bytes=16_000_000),
            name="log_probs",
        )(z, ls, nin)
        return logprobs, log_sum.reshape(rows), next_in

    return jax.shard_map(
        per_device,
        mesh=mesh,
        in_specs=(P("dp", "tp"), P("tp"), P("tp"), P("vp", "tp"), P("dp"), P("tp"), P("tp")),
        out_specs=(P("dp", ("vp", "tp")), P("dp"), P("dp", "tp")),
        check_vma=False,
    )
```

```python
import functools

import jax
import jax.numpy as jnp
from jax import lax
from jax.experimental import pallas as pl
from jax.experimental.pallas import tpu as pltpu
from jax.sharding import PartitionSpec as P

NORM_EPS = 1e-5
LANES = 128
CHUNK = 1024
HEAD = 384
DOT_COLS = 512
PICK = 1280
MESH_ID = pl.DeviceIdType.MESH


def _row_stats(x):
    sums = x[:, :LANES]
    squares = sums * sums
    for c in range(LANES, x.shape[1], LANES):
        part = x[:, c : c + LANES]
        sums = sums + part
        squares = squares + part * part
    both = jnp.concatenate([sums, squares], axis=0)
    return jnp.sum(both.T, axis=0, keepdims=True)


def _as_columns(row):
    return jnp.broadcast_to(row, (LANES, LANES)).T


def _mean_rstd(total, rows, full_width):
    cols = _as_columns(total)
    mean = cols[:rows] / full_width
    var = cols[rows : 2 * rows] / full_width - mean * mean
    return mean, lax.rsqrt(var + NORM_EPS)


def _normalize(x, mean, rstd, gain, bias):
    parts = []
    for c in range(0, x.shape[1], LANES):
        scaled = (x[:, c : c + LANES] - mean) * rstd
        parts.append(scaled * gain[:, c : c + LANES] + bias[:, c : c + LANES])
    return jnp.concatenate(parts, axis=1).astype(jnp.bfloat16)


def _unpacked(packed, first_row, rows_per_group, cols):
    group, r = first_row // rows_per_group, first_row % rows_per_group
    v = packed[r : r + 8, :]
    return pltpu.roll(v, LANES - group * cols, 1) if group else v


def _head_kernel(
    tp_size, vp_size,
    hid_hbm, g1_hbm, b1_hbm, g2_hbm, b2_hbm, tok_hbm, emb,
    z_out, ls_out, nin_out,
    hid, norms, tok,
    e_all, mine, from_peer, to_peer, ring, xn, xn_peer, early, early_out, early_in, early_rows,
    top, acc, e_src, e_in, stat_src, stat_in, lse_src, lse_in,
    small_sem, e_sem, early_sem, peer_send, peer_recv, ring_send, ring_recv,
    stat_send, stat_recv, row_sem, lse_send, lse_recv,
):
    rows, width = hid.shape
    full_width = width * tp_size
    vocab_rows = emb.shape[0]
    own_cols = vocab_rows // tp_size
    chips = tp_size // 2
    n_chunks = pl.cdiv(own_cols, CHUNK)
    half_chunks = n_chunks // 2
    half_cols = half_chunks * CHUNK
    tail = own_cols - (n_chunks - 1) * CHUNK
    rest = tail % LANES
    rest_rows = rows * rest // LANES

    def buffer_rows(cols):
        return cols // LANES * rows + (rest_rows if cols % LANES else 0)

    me = lax.axis_index("tp")
    my_vp = lax.axis_index("vp")
    chip = me // 2
    core = me % 2
    peer = 2 * chip + 1 - core
    turn = 1 - 2 * core

    def chip_at(offset):
        return (chip + offset + chips) % chips

    fwd = 2 * chip_at(turn) + core
    bwd = 2 * chip_at(-turn) + core

    barrier = pltpu.get_barrier_semaphore()
    far_first = sorted(range(1, tp_size), key=lambda j: -min(j, tp_size - j))
    for j in far_first:
        pl.semaphore_signal(barrier, inc=1, device_id={"tp": (me + j) % tp_size}, device_id_type=MESH_ID)
    for j in range(1, vp_size):
        pl.semaphore_signal(barrier, inc=1, device_id={"vp": (my_vp + j) % vp_size}, device_id_type=MESH_ID)

    hid_load = pltpu.make_async_copy(hid_hbm, hid, small_sem.at[0])
    tok_load = pltpu.make_async_copy(tok_hbm, tok, small_sem.at[1])
    hid_load.start()
    for i, src in enumerate([g1_hbm, b1_hbm, g2_hbm, b2_hbm]):
        pltpu.make_async_copy(src, norms.at[i], small_sem.at[2]).start()
    tok_load.start()

    def block_of(phase, half, sign):
        if phase == 0:
            return chip_at(2)
        if phase == 3:
            return chip
        if (phase == 1) == (half == 0):
            return chip_at(-sign)
        return chip_at(sign)

    def first_row(phase, half, own):
        if own:
            return (2 * block_of(phase, half, turn) + core) * own_cols + half * half_cols
        return (2 * block_of(phase, half, -turn) + 1 - core) * own_cols + half * half_cols

    def table_load(phase, half, own):
        count = half_cols if half == 0 else own_cols - half_cols
        span = pl.ds(pl.multiple_of(first_row(phase, half, own), 16), count)
        return pltpu.make_async_copy(emb.at[span], e_all.at[span], e_sem.at[min(phase, 1)])

    def wait_table(phases):
        span = pl.ds(0, 2 * own_cols * phases)
        pltpu.make_async_copy(emb.at[span], e_all.at[span], e_sem.at[min(phases - 1, 1)]).wait()

    for half in range(2):
        rows_at = pl.ds(pl.multiple_of(first_row(0, half, 0), 16), HEAD)
        pltpu.make_async_copy(emb.at[rows_at], early.at[pl.ds(half * HEAD, HEAD)], early_sem.at[0]).start()

    hid_load.wait()
    pltpu.make_async_copy(norms, norms, small_sem.at[2]).wait()
    tok_load.wait()
    for phase in range(4):
        for own in range(2):
            for half in range(2):
                table_load(phase, half, own).start()

    def share(src, dst, send, recv, axis, j):
        size, at = (tp_size, me) if axis == "tp" else (vp_size, my_vp)
        return pltpu.make_async_remote_copy(
            src_ref=src, dst_ref=dst.at[j - 1], send_sem=send, recv_sem=recv,
            device_id={axis: (at + j) % size}, device_id_type=MESH_ID)

    def all_shared(dst, send, recv, axis):
        at = (me + 1) % tp_size if axis == "tp" else (my_vp + 1) % vp_size
        return pltpu.make_async_remote_copy(
            src_ref=dst, dst_ref=dst, send_sem=send, recv_sem=recv,
            device_id={axis: at}, device_id_type=MESH_ID)

    def share_stats(s):
        for j in far_first:
            share(stat_src.at[s], stat_in.at[s], stat_send.at[0], stat_recv.at[s], "tp", j).start()

    def stat_total(s):
        all_shared(stat_in.at[s], stat_send.at[0], stat_recv.at[s], "tp").wait_recv()
        total = stat_src[s]
        for j in range(1, tp_size):
            total = total + stat_in[s, j - 1]
        return total

    x = hid[...].astype(jnp.float32)
    stat_src[0] = _row_stats(x)
    early_out[pl.ds(2 * HEAD, rows), :] = x
    early_out[pl.ds(2 * HEAD + rows, 8), :] = jnp.concatenate(
        [norms[0], norms[1], jnp.zeros((6, width), jnp.float32)], axis=0)
    pltpu.make_async_copy(emb.at[pl.ds(0, 2 * HEAD)], early, early_sem.at[0]).wait()
    early_out[pl.ds(0, 2 * HEAD), :] = early[...].astype(jnp.float32)
    pl.semaphore_wait(barrier, tp_size - 1 + vp_size - 1)
    share_stats(0)
    early_copy = pltpu.make_async_remote_copy(
        src_ref=early_out, dst_ref=early_in, send_sem=early_sem.at[1], recv_sem=early_sem.at[2],
        device_id={"tp": peer}, device_id_type=MESH_ID)
    early_copy.start()
    early_copy.wait_recv()
    early_rows[...] = early_in[pl.ds(0, 2 * HEAD), :].astype(jnp.bfloat16)
    mean, rstd = _mean_rstd(stat_total(0), rows, full_width)
    xn[...] = _normalize(x, mean, rstd, norms[0], norms[1])
    xn_peer[...] = _normalize(
        early_in[pl.ds(2 * HEAD, rows), :], mean, rstd,
        early_in[pl.ds(2 * HEAD + rows, 1), :], early_in[pl.ds(2 * HEAD + rows + 1, 1), :])

    def chunk_dot(dst, base, row0, first, cols):
        for c in range(first, cols, DOT_COLS):
            n = min(DOT_COLS, cols - c)
            part = e_all[pl.ds(pl.multiple_of(row0 + c, 16), n), :]
            v = lax.dot_general(xn[...], part, (((1,), (1,)), ((), ())), preferred_element_type=jnp.float32)
            for t in range(0, n, LANES):
                at = base + (c + t) // LANES * rows
                if t + LANES <= n:
                    dst[pl.ds(at, rows), :] = v[:, t : t + LANES]
                else:
                    dst[pl.ds(at, rest_rows), :] = jnp.concatenate(
                        [v[q : q + rest_rows, t:n] for q in range(0, rows, rest_rows)], axis=1)

    def cols_of(half, last):
        return tail if half == 1 and last else CHUNK

    def at_of(phase, half, k):
        return phase * n_chunks + half * half_chunks + k

    own_rows = buffer_rows(own_cols)

    def base_of(phase, half, k):
        return pl.multiple_of(phase * own_rows + (half * half_chunks + k) * buffer_rows(CHUNK), 8)

    def span_of(phase, half, k, last):
        begin = buffer_rows(HEAD) if phase == 0 and isinstance(k, int) and k == 0 else 0
        return pl.ds(base_of(phase, half, k) + begin, buffer_rows(cols_of(half, last)) - begin)

    def peer_recv_of(phase, k):
        return peer_recv.at[k if phase == 0 else half_chunks + phase - 1]

    def peer_copy(phase, half, k, last):
        span = span_of(phase, half, k, last)
        return pltpu.make_async_remote_copy(
            src_ref=to_peer.at[span], dst_ref=from_peer.at[span],
            send_sem=peer_send.at[0], recv_sem=peer_recv_of(phase, k),
            device_id={"tp": peer}, device_id_type=MESH_ID)

    def wait_peer(recv, count):
        ref = from_peer.at[pl.ds(0, count)]
        pltpu.make_async_remote_copy(
            src_ref=ref, dst_ref=ref, send_sem=peer_send.at[0], recv_sem=recv,
            device_id={"tp": peer}, device_id_type=MESH_ID).wait_recv()

    def wait_peer_phase(phase):
        wait_peer(peer_recv_of(phase, 0), own_rows)

    def wait_peer_chunk(k, last):
        wait_peer(peer_recv_of(0, k), sum(span_of(0, half, k, last).size for half in range(2)))

    def ring_recv_of(phase, half, k):
        return ring_recv.at[phase if phase < 2 else 2 + half * half_chunks + k]

    def ring_copy(phase, half, k, last):
        span = span_of(phase, half, k, last)
        forward = (half == 0) != (phase == 1)
        return pltpu.make_async_remote_copy(
            src_ref=mine.at[span], dst_ref=ring.at[span],
            send_sem=ring_send.at[0], recv_sem=ring_recv_of(phase, half, k),
            device_id={"tp": fwd if forward else bwd}, device_id_type=MESH_ID)

    def whole_phase(ref, phase):
        return ref.at[pl.ds(phase * own_rows, own_rows)]

    def wait_ring_phase(phase):
        ref = whole_phase(ring, phase)
        pltpu.make_async_remote_copy(
            src_ref=ref, dst_ref=ref, send_sem=ring_send.at[0], recv_sem=ring_recv.at[phase],
            device_id={"tp": fwd}, device_id_type=MESH_ID).wait_recv()

    head_rows = pl.ds(0, buffer_rows(HEAD))

    def head_ring_copy(half):
        span = pl.ds(half * half_chunks * buffer_rows(CHUNK), head_rows.size)
        return pltpu.make_async_remote_copy(
            src_ref=mine.at[span], dst_ref=ring.at[span],
            send_sem=ring_send.at[0], recv_sem=ring_recv.at[0],
            device_id={"tp": bwd if half else fwd}, device_id_type=MESH_ID)

    def add_into(base, others, begin, end):
        for r in range(begin, end, 8):
            v = mine[pl.ds(base + r, 8), :]
            for ref, at in others:
                v = v + ref[pl.ds(at + r, 8), :]
            mine[pl.ds(base + r, 8), :] = v

    def to_peer_dot(phase, half, k, last, first=0, end=None):
        chunk_dot(to_peer, base_of(phase, half, k), first_row(phase, half, 0) + k * CHUNK,
                  first, end or cols_of(half, last))

    def mine_dot(phase, half, k, last, first=0, end=None):
        if phase < 3:
            dst, base = mine, base_of(phase, half, k)
        else:
            dst, base = z_out, base_of(0, half, k)
        chunk_dot(dst, base, first_row(phase, half, 1) + k * CHUNK, first, end or cols_of(half, last))

    def first_product():
        for half in range(2):
            part = e_all[pl.ds(pl.multiple_of(first_row(0, half, 1), 16), HEAD), :]
            dims = (((1,), (1,)), ((), ()))
            v = lax.dot_general(xn[...], part, dims, preferred_element_type=jnp.float32) + lax.dot_general(
                xn_peer[...], early_rows[pl.ds(half * HEAD, HEAD), :], dims, preferred_element_type=jnp.float32)
            for t in range(0, HEAD, LANES):
                mine[pl.ds(base_of(0, half, 0) + t // LANES * rows, rows), :] = v[:, t : t + LANES]
        for half in range(2):
            head_ring_copy(half).start()
        for half in range(2):
            to_peer_dot(0, half, 0, False, HEAD)
        for half in range(2):
            peer_copy(0, half, 0, False).start()
        for half in range(2):
            mine_dot(0, half, 0, False, HEAD)
        wait_peer_chunk(0, False)
        for half in range(2):
            at = base_of(0, half, 0)
            add_into(at, [(from_peer, at)], buffer_rows(HEAD), buffer_rows(CHUNK))
        for half in range(2):
            ring_copy(0, half, 0, False).start()

    def join(phase, k, last):
        for half in range(2):
            at = base_of(phase, half, k)
            add_into(at, [(from_peer, at)], 0, buffer_rows(cols_of(half, last)))
        for half in range(2):
            ring_copy(phase, half, k, last).start()

    def product(phase, k, last):
        for half in range(2):
            to_peer_dot(phase, half, k, last)
        for half in range(2):
            peer_copy(phase, half, k, last).start()
        for half in range(2):
            mine_dot(phase, half, k, last)
        if phase == 0:
            wait_peer_chunk(k, last)
            join(phase, k, last)

    def each_chunk(body, begin=0):
        def step(k, carry):
            body(k, False)
            return carry

        for k in range(begin, 1):
            body(k, False)
        lax.fori_loop(1, half_chunks - 1, step, 0)
        body(half_chunks - 1, True)

    wait_table(1)
    first_product()
    each_chunk(functools.partial(product, 0), 1)

    wait_table(3)

    def pick_rows():
        wanted = tok[...].astype(jnp.float32) - (my_vp * vocab_rows).astype(jnp.float32)
        wanted = jnp.concatenate([wanted, jnp.zeros((1, LANES - rows), jnp.float32)], axis=1)
        wanted = _as_columns(wanted)[:rows].astype(jnp.int32)
        lane = lax.broadcasted_iota(jnp.int32, wanted.shape, 1)

        def add(first, count):
            hits = []
            for c in range(0, count, LANES):
                hits.append(jnp.where(lane + (first + c) == wanted, 1.0, 0.0).astype(jnp.bfloat16))
            e_src[...] += jnp.dot(
                jnp.concatenate(hits, axis=1), e_all[pl.ds(pl.multiple_of(first, LANES), count), :],
                preferred_element_type=jnp.float32)

        def step(i, carry):
            add(i * PICK, PICK)
            return carry

        e_src[...] = jnp.zeros_like(e_src)
        lax.fori_loop(0, vocab_rows // PICK, step, 0)
        if vocab_rows % PICK:
            add(vocab_rows // PICK * PICK, vocab_rows % PICK)

    each_chunk(functools.partial(product, 1))
    wait_peer_phase(1)
    each_chunk(functools.partial(join, 1))
    pick_rows()
    for j in range(1, vp_size):
        share(e_src, e_in, row_sem.at[0], row_sem.at[1], "vp", j).start()
    each_chunk(functools.partial(product, 2))

    def token_rows():
        rows_sum = e_src[...]
        for j in range(1, vp_size):
            rows_sum = rows_sum + e_in[j - 1]
        return rows_sum

    all_shared(e_in, row_sem.at[0], row_sem.at[1], "vp").wait()
    stat_src[1] = _row_stats(token_rows())
    share_stats(1)

    def forward_chunk(k, last):
        for half in range(2):
            at = base_of(2, half, k)
            add_into(at, [(from_peer, at), (ring, base_of(0, half, k))], 0, buffer_rows(cols_of(half, last)))
        for half in range(2):
            ring_copy(2, half, k, last).start()

    wait_peer_phase(2)
    wait_ring_phase(0)
    each_chunk(forward_chunk)
    each_chunk(functools.partial(product, 3))
    mean, rstd = _mean_rstd(stat_total(1), rows, full_width)
    nin_out[...] = _normalize(token_rows(), mean, rstd, norms[2], norms[3])

    top[...] = jnp.full(top.shape, jnp.finfo(jnp.float32).min, jnp.float32)
    acc[...] = jnp.zeros_like(acc)

    def finish_chunk(k, last):
        for half in range(2):
            cols = cols_of(half, last)
            base, peer_base = base_of(0, half, k), base_of(3, half, k)
            single, chain = base_of(1, half, k), base_of(2, half, k)
            ring_copy(2, half, k, last).wait_recv()

            def final(r):
                v = (z_out[pl.ds(base + r, 8), :] + from_peer[pl.ds(peer_base + r, 8), :]) + (
                    ring[pl.ds(single + r, 8), :] + ring[pl.ds(chain + r, 8), :])
                z_out[pl.ds(base + r, 8), :] = v
                return v

            full = cols // LANES
            if cols % LANES:
                packed = jnp.concatenate([final(full * rows + r) for r in range(0, rest_rows, 8)], axis=0)
            for r in range(0, rows, 8):
                tiles = [final(t * rows + r) for t in range(full)]
                if cols % LANES:
                    v = _unpacked(packed, r, rest_rows, rest)
                    tiles.append(jnp.where(lax.broadcasted_iota(jnp.int32, v.shape, 1) < rest, v, -jnp.inf))
                old = top[r : r + 8, :]
                best = functools.reduce(jnp.maximum, tiles, old)
                total = acc[r : r + 8, :] * jnp.exp(old - best)
                for v in tiles:
                    total = total + jnp.exp(v - best)
                top[r : r + 8, :] = best
                acc[r : r + 8, :] = total

    wait_peer_phase(3)
    wait_ring_phase(1)
    each_chunk(finish_chunk)

    tops = jnp.concatenate([top[...], top[...]], axis=0).T
    sums = jnp.concatenate([acc[...], acc[...]], axis=0).T
    best = jnp.max(tops, axis=0, keepdims=True)
    total = jnp.sum(sums * jnp.exp(tops - best), axis=0, keepdims=True)

    def merge(best, total, other):
        tops = [best] + [other[j, 0:1, :] for j in range(other.shape[0])]
        sums = [total] + [other[j, 1:2, :] for j in range(other.shape[0])]
        new = functools.reduce(jnp.maximum, tops)
        return new, functools.reduce(jnp.add, [t * jnp.exp(b - new) for b, t in zip(tops, sums)])

    vp_far_first = sorted(range(1, vp_size), key=lambda j: -min(j, vp_size - j))
    stages = (
        ("tp", far_first, lse_in.at[pl.ds(0, tp_size - 1)]),
        ("vp", vp_far_first, lse_in.at[pl.ds(tp_size - 1, vp_size - 1)]))
    for i, (axis, order, other) in enumerate(stages):
        lse_src[i, 0:1, :] = best
        lse_src[i, 1:2, :] = total
        for j in order:
            share(lse_src.at[i], other, lse_send.at[0], lse_recv.at[i], axis, j).start()
        all_shared(other, lse_send.at[0], lse_recv.at[i], axis).wait_recv()
        best, total = merge(best, total, other)
    ls_out[...] = jnp.broadcast_to(best + jnp.log(total), ls_out.shape)

    early_copy.wait_send()
    all_shared(stat_in, stat_send.at[0], stat_recv.at[0], "tp").wait_send()
    all_shared(lse_in, lse_send.at[0], lse_recv.at[0], "tp").wait_send()
    sent_to_peer = to_peer.at[pl.ds(0, 4 * own_rows - 2 * buffer_rows(HEAD))]
    for ref, sem in ((mine, ring_send), (sent_to_peer, peer_send)):
        pltpu.make_async_remote_copy(
            src_ref=ref, dst_ref=ref, send_sem=sem.at[0], recv_sem=ring_recv.at[0],
            device_id={"tp": peer}, device_id_type=MESH_ID).wait_send()


def _subtract_kernel(z, ls, nin, logprobs, log_sum, next_in, out, sums, sems):
    rows, n = out.shape
    rest = n % LANES
    rest_rows = rows * rest // LANES
    step = rows // 4
    copies = [
        pltpu.make_async_copy(nin, next_in, sems.at[4]),
        pltpu.make_async_copy(sums, log_sum, sems.at[5]),
    ]
    copies[0].start()
    sums[...] = ls[0:1, :rows]
    cols = _as_columns(ls[0:1, :])[:rows]
    packed = z[n // LANES * rows :, :]
    for i in range(4):
        for r in range(i * step, (i + 1) * step, 8):
            for t in range(n // LANES):
                out[r : r + 8, t * LANES : (t + 1) * LANES] = z[t * rows + r : t * rows + r + 8, :] - cols[r : r + 8]
            if rest:
                v = _unpacked(packed, r, rest_rows, rest) - cols[r : r + 8]
                out[r : r + 8, n - rest :] = v[:, :rest]
        span = pl.ds(i * step, step)
        copies.append(pltpu.make_async_copy(out.at[span], logprobs.at[span], sems.at[i]))
        copies[-1].start()
        if i == 0:
            copies[1].start()
    for copy in copies:
        copy.wait()


def solution(mesh):
    tp_size = mesh.shape["tp"]
    vp_size = mesh.shape["vp"]

    def per_device(hidden, lnf_gain, lnf_bias, emb_table, next_tok, eln_gain, eln_bias):
        rows, width = hidden.shape
        own_cols = emb_table.shape[0] // tp_size
        n_chunks = pl.cdiv(own_cols, CHUNK)
        f32 = jnp.float32
        vmem = pl.BlockSpec(memory_space=pltpu.VMEM)
        hbm = pl.BlockSpec(memory_space=pltpu.HBM)
        dma = pltpu.SemaphoreType.DMA
        own_rows = rows * own_cols // LANES
        z, ls, nin = pl.pallas_call(
            functools.partial(_head_kernel, tp_size, vp_size),
            out_shape=(
                pltpu.VMEM((own_rows, LANES), f32),
                pltpu.VMEM((8, LANES), f32),
                pltpu.VMEM((rows, width), jnp.bfloat16),
            ),
            in_specs=[hbm] * 7,
            out_specs=(vmem,) * 3,
            scratch_shapes=[
                pltpu.VMEM((rows, width), hidden.dtype),
                pltpu.VMEM((4, 1, width), f32),
                pltpu.VMEM((1, rows), jnp.int32),
                pltpu.VMEM(emb_table.shape, emb_table.dtype),
                pltpu.VMEM((3 * own_rows, LANES), f32),
                pltpu.VMEM((4 * own_rows, LANES), f32),
                pltpu.VMEM((4 * own_rows, LANES), f32),
                pltpu.VMEM((3 * own_rows, LANES), f32),
                pltpu.VMEM((rows, width), jnp.bfloat16),
                pltpu.VMEM((rows, width), jnp.bfloat16),
                pltpu.VMEM((2 * HEAD, width), emb_table.dtype),
                pltpu.VMEM((2 * HEAD + rows + 8, width), f32),
                pltpu.VMEM((2 * HEAD + rows + 8, width), f32),
                pltpu.VMEM((2 * HEAD, width), emb_table.dtype),
                pltpu.VMEM((rows, LANES), f32),
                pltpu.VMEM((rows, LANES), f32),
                pltpu.VMEM((rows, width), f32),
                pltpu.VMEM((vp_size - 1, rows, width), f32),
                pltpu.VMEM((2, 1, LANES), f32),
                pltpu.VMEM((2, tp_size - 1, 1, LANES), f32),
                pltpu.VMEM((2, 2, LANES), f32),
                pltpu.VMEM((tp_size - 1 + vp_size - 1, 2, LANES), f32),
                dma((3,)),
                dma((2,)),
                dma((3,)),
                dma((1,)),
                dma((n_chunks // 2 + 3,)),
                dma((1,)),
                dma((2 + n_chunks,)),
                dma((1,)),
                dma((2,)),
                dma((2,)),
                dma((1,)),
                dma((2,)),
            ],
            compiler_params=pltpu.CompilerParams(
                collective_id=0, has_side_effects=True, vmem_limit_bytes=64_500_000),
            name="vocab_head",
        )(
            hidden, lnf_gain.reshape(1, width), lnf_bias.reshape(1, width),
            eln_gain.reshape(1, width), eln_bias.reshape(1, width), next_tok.reshape(1, rows), emb_table,
        )
        logprobs, log_sum, next_in = pl.pallas_call(
            _subtract_kernel,
            out_shape=(
                jax.ShapeDtypeStruct((rows, own_cols), f32),
                jax.ShapeDtypeStruct((1, rows), f32),
                jax.ShapeDtypeStruct((rows, width), jnp.bfloat16),
            ),
            in_specs=[vmem] * 3,
            out_specs=(hbm,) * 3,
            scratch_shapes=[pltpu.VMEM((rows, own_cols), f32), pltpu.VMEM((1, rows), f32), dma((6,))],
            compiler_params=pltpu.CompilerParams(vmem_limit_bytes=16_000_000),
            name="log_probs",
        )(z, ls, nin)
        return logprobs, log_sum.reshape(rows), next_in

    return jax.shard_map(
        per_device,
        mesh=mesh,
        in_specs=(P("dp", "tp"), P("tp"), P("tp"), P("vp", "tp"), P("dp"), P("tp"), P("tp")),
        out_specs=(P("dp", ("vp", "tp")), P("dp"), P("dp", "tp")),
        check_vma=False,
    )
```

```python
import functools

import jax
import jax.numpy as jnp
from jax import lax
from jax.experimental import pallas as pl
from jax.experimental.pallas import tpu as pltpu
from jax.sharding import PartitionSpec as P

NORM_EPS = 1e-5
LANES = 128
CHUNK = 1024
HEAD = 512
HEAD_STEP = 128
DOT_COLS = 512
PICK = 1280
MESH_ID = pl.DeviceIdType.MESH


def _row_stats(x):
    sums = x[:, :LANES]
    squares = sums * sums
    for c in range(LANES, x.shape[1], LANES):
        part = x[:, c : c + LANES]
        sums = sums + part
        squares = squares + part * part
    both = jnp.concatenate([sums, squares], axis=0)
    return jnp.sum(both.T, axis=0, keepdims=True)


def _as_columns(row):
    return jnp.broadcast_to(row, (LANES, LANES)).T


def _mean_rstd(total, rows, full_width):
    cols = _as_columns(total)
    mean = cols[:rows] / full_width
    var = cols[rows : 2 * rows] / full_width - mean * mean
    return mean, lax.rsqrt(var + NORM_EPS)


def _normalize(x, mean, rstd, gain, bias):
    parts = []
    for c in range(0, x.shape[1], LANES):
        scaled = (x[:, c : c + LANES] - mean) * rstd
        parts.append(scaled * gain[:, c : c + LANES] + bias[:, c : c + LANES])
    return jnp.concatenate(parts, axis=1).astype(jnp.bfloat16)


def _unpacked(packed, first_row, rows_per_group, cols):
    group, r = first_row // rows_per_group, first_row % rows_per_group
    v = packed[r : r + 8, :]
    return pltpu.roll(v, LANES - group * cols, 1) if group else v


def _head_kernel(
    tp_size, vp_size,
    hid_hbm, g1_hbm, b1_hbm, g2_hbm, b2_hbm, tok_hbm, emb,
    z_out, ls_out, nin_out,
    hid, norms, tok,
    e_all, mine, from_peer, to_peer, ring, xn, xn_peer, early_out, early_in, early_rows,
    top, acc, e_src, e_in, stat_src, stat_in, lse_src, lse_in,
    small_sem, e_sem, early_sem, peer_send, peer_recv, ring_send, ring_recv,
    stat_send, stat_recv, row_sem, lse_send, lse_recv,
):
    rows, width = hid.shape
    full_width = width * tp_size
    vocab_rows = emb.shape[0]
    own_cols = vocab_rows // tp_size
    chips = tp_size // 2
    n_chunks = pl.cdiv(own_cols, CHUNK)
    half_chunks = n_chunks // 2
    half_cols = half_chunks * CHUNK
    tail = own_cols - (n_chunks - 1) * CHUNK
    rest = tail % LANES
    rest_rows = rows * rest // LANES

    def buffer_rows(cols):
        return cols // LANES * rows + (rest_rows if cols % LANES else 0)

    me = lax.axis_index("tp")
    my_vp = lax.axis_index("vp")
    chip = me // 2
    core = me % 2
    peer = 2 * chip + 1 - core
    turn = 1 - 2 * core

    def chip_at(offset):
        return (chip + offset + chips) % chips

    fwd = 2 * chip_at(turn) + core
    bwd = 2 * chip_at(-turn) + core

    barrier = pltpu.get_barrier_semaphore()
    def tp_peer(j):
        return 2 * chip_at(j // 2) + (core if j % 2 == 0 else 1 - core)

    far_first = sorted(range(1, tp_size), key=lambda j: -min(j // 2, chips - j // 2))
    for j in far_first:
        pl.semaphore_signal(barrier, inc=1, device_id={"tp": tp_peer(j)}, device_id_type=MESH_ID)
    for j in range(1, vp_size):
        pl.semaphore_signal(barrier, inc=1, device_id={"vp": (my_vp + j) % vp_size}, device_id_type=MESH_ID)

    hid_load = pltpu.make_async_copy(hid_hbm, hid, small_sem.at[0])
    tok_load = pltpu.make_async_copy(tok_hbm, tok, small_sem.at[1])
    hid_load.start()
    for i, src in enumerate([g1_hbm, b1_hbm, g2_hbm, b2_hbm]):
        pltpu.make_async_copy(src, norms.at[i], small_sem.at[2]).start()
    tok_load.start()

    def block_of(phase, half, sign):
        if phase == 0:
            return chip_at(2)
        if phase == 3:
            return chip
        if (phase == 1) == (half == 0):
            return chip_at(-sign)
        return chip_at(sign)

    def first_row(phase, half, own):
        if own:
            return (2 * block_of(phase, half, turn) + core) * own_cols + half * half_cols
        return (2 * block_of(phase, half, -turn) + 1 - core) * own_cols + half * half_cols

    def table_load(phase, half, own):
        count = half_cols if half == 0 else own_cols - half_cols
        span = pl.ds(pl.multiple_of(first_row(phase, half, own), 16), count)
        return pltpu.make_async_copy(emb.at[span], e_all.at[span], e_sem.at[min(phase, 1)])

    def wait_table(phases):
        span = pl.ds(0, 2 * own_cols * phases)
        pltpu.make_async_copy(emb.at[span], e_all.at[span], e_sem.at[min(phases - 1, 1)]).wait()

    for half in range(2):
        rows_at = pl.ds(pl.multiple_of(first_row(0, half, 0), 16), HEAD)
        pltpu.make_async_copy(emb.at[rows_at], early_rows.at[pl.ds(half * HEAD, HEAD)], early_sem.at[0]).start()

    hid_load.wait()
    pltpu.make_async_copy(norms, norms, small_sem.at[2]).wait()
    tok_load.wait()
    for phase in range(4):
        for own in range(2):
            for half in range(2):
                table_load(phase, half, own).start()

    def share(src, dst, send, recv, axis, j):
        to = tp_peer(j) if axis == "tp" else (my_vp + j) % vp_size
        return pltpu.make_async_remote_copy(
            src_ref=src, dst_ref=dst.at[j - 1], send_sem=send, recv_sem=recv,
            device_id={axis: to}, device_id_type=MESH_ID)

    def all_shared(dst, send, recv, axis):
        at = (me + 1) % tp_size if axis == "tp" else (my_vp + 1) % vp_size
        return pltpu.make_async_remote_copy(
            src_ref=dst, dst_ref=dst, send_sem=send, recv_sem=recv,
            device_id={axis: at}, device_id_type=MESH_ID)

    def share_stats(s):
        for j in far_first:
            share(stat_src.at[s], stat_in.at[s], stat_send.at[0], stat_recv.at[s], "tp", j).start()

    def stat_total(s):
        all_shared(stat_in.at[s], stat_send.at[0], stat_recv.at[s], "tp").wait_recv()
        total = stat_src[s]
        for j in range(1, tp_size):
            total = total + stat_in[s, j - 1]
        return total

    x = hid[...].astype(jnp.float32)
    stat_src[0] = _row_stats(x)
    pl.semaphore_wait(barrier, tp_size - 1 + vp_size - 1)
    share_stats(0)
    early_out[pl.ds(2 * HEAD, rows), :] = x
    early_out[pl.ds(2 * HEAD + rows, 8), :] = jnp.concatenate(
        [norms[0], norms[1], jnp.zeros((6, width), jnp.float32)], axis=0)
    pltpu.make_async_copy(emb.at[pl.ds(0, 2 * HEAD)], early_rows, early_sem.at[0]).wait()
    early_out[pl.ds(0, 2 * HEAD), :] = early_rows[...].astype(jnp.float32)
    early_copy = pltpu.make_async_remote_copy(
        src_ref=early_out, dst_ref=early_in, send_sem=early_sem.at[1], recv_sem=early_sem.at[2],
        device_id={"tp": peer}, device_id_type=MESH_ID)
    early_copy.start()
    early_copy.wait_recv()
    early_rows[...] = early_in[pl.ds(0, 2 * HEAD), :].astype(jnp.bfloat16)
    mean, rstd = _mean_rstd(stat_total(0), rows, full_width)
    xn[...] = _normalize(x, mean, rstd, norms[0], norms[1])
    xn_peer[...] = _normalize(
        early_in[pl.ds(2 * HEAD, rows), :], mean, rstd,
        early_in[pl.ds(2 * HEAD + rows, 1), :], early_in[pl.ds(2 * HEAD + rows + 1, 1), :])

    def chunk_dot(dst, base, row0, first, cols):
        for c in range(first, cols, DOT_COLS):
            n = min(DOT_COLS, cols - c)
            part = e_all[pl.ds(pl.multiple_of(row0 + c, 16), n), :]
            v = lax.dot_general(xn[...], part, (((1,), (1,)), ((), ())), preferred_element_type=jnp.float32)
            for t in range(0, n, LANES):
                at = base + (c + t) // LANES * rows
                if t + LANES <= n:
                    dst[pl.ds(at, rows), :] = v[:, t : t + LANES]
                else:
                    dst[pl.ds(at, rest_rows), :] = jnp.concatenate(
                        [v[q : q + rest_rows, t:n] for q in range(0, rows, rest_rows)], axis=1)

    def cols_of(half, last):
        return tail if half == 1 and last else CHUNK

    def at_of(phase, half, k):
        return phase * n_chunks + half * half_chunks + k

    own_rows = buffer_rows(own_cols)

    def base_of(phase, half, k):
        return pl.multiple_of(phase * own_rows + (half * half_chunks + k) * buffer_rows(CHUNK), 8)

    def span_of(phase, half, k, last):
        begin = buffer_rows(HEAD) if phase == 0 and isinstance(k, int) and k == 0 else 0
        return pl.ds(base_of(phase, half, k) + begin, buffer_rows(cols_of(half, last)) - begin)

    def peer_recv_of(phase, k):
        return peer_recv.at[k if phase == 0 else half_chunks + phase - 1]

    def peer_copy(phase, half, k, last):
        span = span_of(phase, half, k, last)
        return pltpu.make_async_remote_copy(
            src_ref=to_peer.at[span], dst_ref=from_peer.at[span],
            send_sem=peer_send.at[0], recv_sem=peer_recv_of(phase, k),
            device_id={"tp": peer}, device_id_type=MESH_ID)

    def wait_peer(recv, count):
        ref = from_peer.at[pl.ds(0, count)]
        pltpu.make_async_remote_copy(
            src_ref=ref, dst_ref=ref, send_sem=peer_send.at[0], recv_sem=recv,
            device_id={"tp": peer}, device_id_type=MESH_ID).wait_recv()

    def wait_peer_phase(phase):
        wait_peer(peer_recv_of(phase, 0), own_rows)

    def wait_peer_chunk(k, last):
        wait_peer(peer_recv_of(0, k), sum(span_of(0, half, k, last).size for half in range(2)))

    def ring_recv_of(phase, half, k):
        return ring_recv.at[phase if phase < 2 else 2 + half * half_chunks + k]

    def ring_copy(phase, half, k, last):
        span = span_of(phase, half, k, last)
        forward = (half == 0) != (phase == 1)
        return pltpu.make_async_remote_copy(
            src_ref=mine.at[span], dst_ref=ring.at[span],
            send_sem=ring_send.at[0], recv_sem=ring_recv_of(phase, half, k),
            device_id={"tp": fwd if forward else bwd}, device_id_type=MESH_ID)

    def whole_phase(ref, phase):
        return ref.at[pl.ds(phase * own_rows, own_rows)]

    def wait_ring_phase(phase):
        ref = whole_phase(ring, phase)
        pltpu.make_async_remote_copy(
            src_ref=ref, dst_ref=ref, send_sem=ring_send.at[0], recv_sem=ring_recv.at[phase],
            device_id={"tp": fwd}, device_id_type=MESH_ID).wait_recv()

    def head_ring_copy(half, c):
        span = pl.ds(half * half_chunks * buffer_rows(CHUNK) + buffer_rows(c), buffer_rows(HEAD_STEP))
        return pltpu.make_async_remote_copy(
            src_ref=mine.at[span], dst_ref=ring.at[span],
            send_sem=ring_send.at[0], recv_sem=ring_recv.at[0],
            device_id={"tp": bwd if half else fwd}, device_id_type=MESH_ID)

    def add_into(base, others, begin, end):
        for r in range(begin, end, 8):
            v = mine[pl.ds(base + r, 8), :]
            for ref, at in others:
                v = v + ref[pl.ds(at + r, 8), :]
            mine[pl.ds(base + r, 8), :] = v

    def to_peer_dot(phase, half, k, last, first=0, end=None):
        chunk_dot(to_peer, base_of(phase, half, k), first_row(phase, half, 0) + k * CHUNK,
                  first, end or cols_of(half, last))

    def mine_dot(phase, half, k, last, first=0, end=None):
        if phase < 3:
            dst, base = mine, base_of(phase, half, k)
        else:
            dst, base = z_out, base_of(0, half, k)
        chunk_dot(dst, base, first_row(phase, half, 1) + k * CHUNK, first, end or cols_of(half, last))

    def first_product():
        dims = (((1,), (1,)), ((), ()))
        for c in range(0, HEAD, HEAD_STEP):
            for half in range(2):
                part = e_all[pl.ds(pl.multiple_of(first_row(0, half, 1) + c, 16), HEAD_STEP), :]
                v = lax.dot_general(xn[...], part, dims, preferred_element_type=jnp.float32) + lax.dot_general(
                    xn_peer[...], early_rows[pl.ds(half * HEAD + c, HEAD_STEP), :], dims,
                    preferred_element_type=jnp.float32)
                for t in range(0, HEAD_STEP, LANES):
                    mine[pl.ds(base_of(0, half, 0) + (c + t) // LANES * rows, rows), :] = v[:, t : t + LANES]
            for half in range(2):
                head_ring_copy(half, c).start()
        for half in range(2):
            to_peer_dot(0, half, 0, False, HEAD)
        for half in range(2):
            peer_copy(0, half, 0, False).start()
        for half in range(2):
            mine_dot(0, half, 0, False, HEAD)
        wait_peer_chunk(0, False)
        for half in range(2):
            at = base_of(0, half, 0)
            add_into(at, [(from_peer, at)], buffer_rows(HEAD), buffer_rows(CHUNK))
        for half in range(2):
            ring_copy(0, half, 0, False).start()

    def join(phase, k, last):
        for half in range(2):
            at = base_of(phase, half, k)
            add_into(at, [(from_peer, at)], 0, buffer_rows(cols_of(half, last)))
        for half in range(2):
            ring_copy(phase, half, k, last).start()

    def product(phase, k, last):
        for half in range(2):
            to_peer_dot(phase, half, k, last)
        for half in range(2):
            peer_copy(phase, half, k, last).start()
        for half in range(2):
            mine_dot(phase, half, k, last)
        if phase == 0:
            wait_peer_chunk(k, last)
            join(phase, k, last)

    def each_chunk(body, begin=0):
        def step(k, carry):
            body(k, False)
            return carry

        for k in range(begin, 1):
            body(k, False)
        lax.fori_loop(1, half_chunks - 1, step, 0)
        body(half_chunks - 1, True)

    wait_table(1)
    first_product()
    each_chunk(functools.partial(product, 0), 1)

    wait_table(3)

    def pick_rows():
        wanted = tok[...].astype(jnp.float32) - (my_vp * vocab_rows).astype(jnp.float32)
        wanted = jnp.concatenate([wanted, jnp.zeros((1, LANES - rows), jnp.float32)], axis=1)
        wanted = _as_columns(wanted)[:rows].astype(jnp.int32)
        lane = lax.broadcasted_iota(jnp.int32, wanted.shape, 1)

        def add(first, count):
            hits = []
            for c in range(0, count, LANES):
                hits.append(jnp.where(lane + (first + c) == wanted, 1.0, 0.0).astype(jnp.bfloat16))
            e_src[...] += jnp.dot(
                jnp.concatenate(hits, axis=1), e_all[pl.ds(pl.multiple_of(first, LANES), count), :],
                preferred_element_type=jnp.float32)

        def step(i, carry):
            add(i * PICK, PICK)
            return carry

        e_src[...] = jnp.zeros_like(e_src)
        lax.fori_loop(0, vocab_rows // PICK, step, 0)
        if vocab_rows % PICK:
            add(vocab_rows // PICK * PICK, vocab_rows % PICK)

    each_chunk(functools.partial(product, 1))
    wait_peer_phase(1)
    each_chunk(functools.partial(join, 1))
    pick_rows()
    for j in range(1, vp_size):
        share(e_src, e_in, row_sem.at[0], row_sem.at[1], "vp", j).start()
    each_chunk(functools.partial(product, 2))

    def token_rows():
        rows_sum = e_src[...]
        for j in range(1, vp_size):
            rows_sum = rows_sum + e_in[j - 1]
        return rows_sum

    all_shared(e_in, row_sem.at[0], row_sem.at[1], "vp").wait()
    stat_src[1] = _row_stats(token_rows())
    share_stats(1)

    def forward_chunk(k, last):
        for half in range(2):
            at = base_of(2, half, k)
            add_into(at, [(from_peer, at), (ring, base_of(0, half, k))], 0, buffer_rows(cols_of(half, last)))
        for half in range(2):
            ring_copy(2, half, k, last).start()

    wait_peer_phase(2)
    wait_ring_phase(0)
    each_chunk(forward_chunk)
    each_chunk(functools.partial(product, 3))
    mean, rstd = _mean_rstd(stat_total(1), rows, full_width)
    nin_out[...] = _normalize(token_rows(), mean, rstd, norms[2], norms[3])

    top[...] = jnp.full(top.shape, jnp.finfo(jnp.float32).min, jnp.float32)
    acc[...] = jnp.zeros_like(acc)

    def finish_chunk(k, last):
        for half in range(2):
            cols = cols_of(half, last)
            base, peer_base = base_of(0, half, k), base_of(3, half, k)
            single, chain = base_of(1, half, k), base_of(2, half, k)
            ring_copy(2, half, k, last).wait_recv()

            def final(r):
                v = (z_out[pl.ds(base + r, 8), :] + from_peer[pl.ds(peer_base + r, 8), :]) + (
                    ring[pl.ds(single + r, 8), :] + ring[pl.ds(chain + r, 8), :])
                z_out[pl.ds(base + r, 8), :] = v
                return v

            full = cols // LANES
            if cols % LANES:
                packed = jnp.concatenate([final(full * rows + r) for r in range(0, rest_rows, 8)], axis=0)
            for r in range(0, rows, 8):
                tiles = [final(t * rows + r) for t in range(full)]
                if cols % LANES:
                    v = _unpacked(packed, r, rest_rows, rest)
                    tiles.append(jnp.where(lax.broadcasted_iota(jnp.int32, v.shape, 1) < rest, v, -jnp.inf))
                old = top[r : r + 8, :]
                best = functools.reduce(jnp.maximum, tiles, old)
                total = acc[r : r + 8, :] * jnp.exp(old - best)
                for v in tiles:
                    total = total + jnp.exp(v - best)
                top[r : r + 8, :] = best
                acc[r : r + 8, :] = total

    wait_peer_phase(3)
    wait_ring_phase(1)
    each_chunk(finish_chunk)

    tops = jnp.concatenate([top[...], top[...]], axis=0).T
    sums = jnp.concatenate([acc[...], acc[...]], axis=0).T
    best = jnp.max(tops, axis=0, keepdims=True)
    total = jnp.sum(sums * jnp.exp(tops - best), axis=0, keepdims=True)

    def merge(best, total, other):
        tops = [best] + [other[j, 0:1, :] for j in range(other.shape[0])]
        sums = [total] + [other[j, 1:2, :] for j in range(other.shape[0])]
        new = functools.reduce(jnp.maximum, tops)
        return new, functools.reduce(jnp.add, [t * jnp.exp(b - new) for b, t in zip(tops, sums)])

    vp_far_first = sorted(range(1, vp_size), key=lambda j: -min(j, vp_size - j))
    stages = (
        ("tp", far_first, lse_in.at[pl.ds(0, tp_size - 1)]),
        ("vp", vp_far_first, lse_in.at[pl.ds(tp_size - 1, vp_size - 1)]))
    for i, (axis, order, other) in enumerate(stages):
        lse_src[i, 0:1, :] = best
        lse_src[i, 1:2, :] = total
        for j in order:
            share(lse_src.at[i], other, lse_send.at[0], lse_recv.at[i], axis, j).start()
        all_shared(other, lse_send.at[0], lse_recv.at[i], axis).wait_recv()
        best, total = merge(best, total, other)
    ls_out[...] = jnp.broadcast_to(best + jnp.log(total), ls_out.shape)

    early_copy.wait_send()
    all_shared(stat_in, stat_send.at[0], stat_recv.at[0], "tp").wait_send()
    all_shared(lse_in, lse_send.at[0], lse_recv.at[0], "tp").wait_send()
    sent_to_peer = to_peer.at[pl.ds(0, 4 * own_rows - 2 * buffer_rows(HEAD))]
    for ref, sem in ((mine, ring_send), (sent_to_peer, peer_send)):
        pltpu.make_async_remote_copy(
            src_ref=ref, dst_ref=ref, send_sem=sem.at[0], recv_sem=ring_recv.at[0],
            device_id={"tp": peer}, device_id_type=MESH_ID).wait_send()


def _subtract_kernel(z, ls, nin, logprobs, log_sum, next_in, out, sums, sems):
    rows, n = out.shape
    rest = n % LANES
    rest_rows = rows * rest // LANES
    step = rows // 4
    copies = [
        pltpu.make_async_copy(nin, next_in, sems.at[4]),
        pltpu.make_async_copy(sums, log_sum, sems.at[5]),
    ]
    copies[0].start()
    sums[...] = ls[0:1, :rows]
    cols = _as_columns(ls[0:1, :])[:rows]
    packed = z[n // LANES * rows :, :]
    for i in range(4):
        for r in range(i * step, (i + 1) * step, 8):
            for t in range(n // LANES):
                out[r : r + 8, t * LANES : (t + 1) * LANES] = z[t * rows + r : t * rows + r + 8, :] - cols[r : r + 8]
            if rest:
                v = _unpacked(packed, r, rest_rows, rest) - cols[r : r + 8]
                out[r : r + 8, n - rest :] = v[:, :rest]
        span = pl.ds(i * step, step)
        copies.append(pltpu.make_async_copy(out.at[span], logprobs.at[span], sems.at[i]))
        copies[-1].start()
        if i == 0:
            copies[1].start()
    for copy in copies:
        copy.wait()


def solution(mesh):
    tp_size = mesh.shape["tp"]
    vp_size = mesh.shape["vp"]

    def per_device(hidden, lnf_gain, lnf_bias, emb_table, next_tok, eln_gain, eln_bias):
        rows, width = hidden.shape
        own_cols = emb_table.shape[0] // tp_size
        n_chunks = pl.cdiv(own_cols, CHUNK)
        f32 = jnp.float32
        vmem = pl.BlockSpec(memory_space=pltpu.VMEM)
        hbm = pl.BlockSpec(memory_space=pltpu.HBM)
        dma = pltpu.SemaphoreType.DMA
        own_rows = rows * own_cols // LANES
        z, ls, nin = pl.pallas_call(
            functools.partial(_head_kernel, tp_size, vp_size),
            out_shape=(
                pltpu.VMEM((own_rows, LANES), f32),
                pltpu.VMEM((8, LANES), f32),
                pltpu.VMEM((rows, width), jnp.bfloat16),
            ),
            in_specs=[hbm] * 7,
            out_specs=(vmem,) * 3,
            scratch_shapes=[
                pltpu.VMEM((rows, width), hidden.dtype),
                pltpu.VMEM((4, 1, width), f32),
                pltpu.VMEM((1, rows), jnp.int32),
                pltpu.VMEM(emb_table.shape, emb_table.dtype),
                pltpu.VMEM((3 * own_rows, LANES), f32),
                pltpu.VMEM((4 * own_rows, LANES), f32),
                pltpu.VMEM((4 * own_rows, LANES), f32),
                pltpu.VMEM((3 * own_rows, LANES), f32),
                pltpu.VMEM((rows, width), jnp.bfloat16),
                pltpu.VMEM((rows, width), jnp.bfloat16),
                pltpu.VMEM((2 * HEAD + rows + 8, width), f32),
                pltpu.VMEM((2 * HEAD + rows + 8, width), f32),
                pltpu.VMEM((2 * HEAD, width), emb_table.dtype),
                pltpu.VMEM((rows, LANES), f32),
                pltpu.VMEM((rows, LANES), f32),
                pltpu.VMEM((rows, width), f32),
                pltpu.VMEM((vp_size - 1, rows, width), f32),
                pltpu.VMEM((2, 1, LANES), f32),
                pltpu.VMEM((2, tp_size - 1, 1, LANES), f32),
                pltpu.VMEM((2, 2, LANES), f32),
                pltpu.VMEM((tp_size - 1 + vp_size - 1, 2, LANES), f32),
                dma((3,)),
                dma((2,)),
                dma((3,)),
                dma((1,)),
                dma((n_chunks // 2 + 3,)),
                dma((1,)),
                dma((2 + n_chunks,)),
                dma((1,)),
                dma((2,)),
                dma((2,)),
                dma((1,)),
                dma((2,)),
            ],
            compiler_params=pltpu.CompilerParams(
                collective_id=0, has_side_effects=True, vmem_limit_bytes=64_500_000),
            name="vocab_head",
        )(
            hidden, lnf_gain.reshape(1, width), lnf_bias.reshape(1, width),
            eln_gain.reshape(1, width), eln_bias.reshape(1, width), next_tok.reshape(1, rows), emb_table,
        )
        logprobs, log_sum, next_in = pl.pallas_call(
            _subtract_kernel,
            out_shape=(
                jax.ShapeDtypeStruct((rows, own_cols), f32),
                jax.ShapeDtypeStruct((1, rows), f32),
                jax.ShapeDtypeStruct((rows, width), jnp.bfloat16),
            ),
            in_specs=[vmem] * 3,
            out_specs=(hbm,) * 3,
            scratch_shapes=[pltpu.VMEM((rows, own_cols), f32), pltpu.VMEM((1, rows), f32), dma((6,))],
            compiler_params=pltpu.CompilerParams(vmem_limit_bytes=16_000_000),
            name="log_probs",
        )(z, ls, nin)
        return logprobs, log_sum.reshape(rows), next_in

    return jax.shard_map(
        per_device,
        mesh=mesh,
        in_specs=(P("dp", "tp"), P("tp"), P("tp"), P("vp", "tp"), P("dp"), P("tp"), P("tp")),
        out_specs=(P("dp", ("vp", "tp")), P("dp"), P("dp", "tp")),
        check_vma=False,
    )
```

```python
import functools

import jax
import jax.numpy as jnp
from jax import lax
from jax.experimental import pallas as pl
from jax.experimental.pallas import tpu as pltpu
from jax.sharding import PartitionSpec as P

NORM_EPS = 1e-5
LANES = 128
CHUNK = 1024
HEAD = 512
HEAD_STEP = 128
DOT_COLS = 512
PICK = 1280
MESH_ID = pl.DeviceIdType.MESH


def _row_stats(x):
    sums = x[:, :LANES]
    squares = sums * sums
    for c in range(LANES, x.shape[1], LANES):
        part = x[:, c : c + LANES]
        sums = sums + part
        squares = squares + part * part
    both = jnp.concatenate([sums, squares], axis=0)
    return jnp.sum(both.T, axis=0, keepdims=True)


def _as_columns(row):
    return jnp.broadcast_to(row, (LANES, LANES)).T


def _mean_rstd(total, rows, full_width):
    cols = _as_columns(total)
    mean = cols[:rows] / full_width
    var = cols[rows : 2 * rows] / full_width - mean * mean
    return mean, lax.rsqrt(var + NORM_EPS)


def _normalize(x, mean, rstd, gain, bias):
    parts = []
    for c in range(0, x.shape[1], LANES):
        scaled = (x[:, c : c + LANES] - mean) * rstd
        parts.append(scaled * gain[:, c : c + LANES] + bias[:, c : c + LANES])
    return jnp.concatenate(parts, axis=1).astype(jnp.bfloat16)


def _unpacked(packed, first_row, rows_per_group, cols):
    group, r = first_row // rows_per_group, first_row % rows_per_group
    v = packed[r : r + 8, :]
    return pltpu.roll(v, LANES - group * cols, 1) if group else v


def _head_kernel(
    tp_size, vp_size,
    hid_hbm, g1_hbm, b1_hbm, g2_hbm, b2_hbm, tok_hbm, emb,
    z_out, ls_out, nin_out,
    hid, norms, tok,
    e_all, mine, from_peer, to_peer, ring, xn, xn_peer, early_out, early_in, early_rows,
    top, acc, e_src, e_in, stat_src, stat_in, lse_src, lse_in,
    small_sem, e_sem, early_sem, peer_send, peer_recv, ring_send, ring_recv,
    stat_send, stat_recv, row_sem, lse_send, lse_recv,
):
    rows, width = hid.shape
    full_width = width * tp_size
    vocab_rows = emb.shape[0]
    own_cols = vocab_rows // tp_size
    chips = tp_size // 2
    n_chunks = pl.cdiv(own_cols, CHUNK)
    half_chunks = n_chunks // 2
    half_cols = half_chunks * CHUNK
    tail = own_cols - (n_chunks - 1) * CHUNK
    rest = tail % LANES
    rest_rows = rows * rest // LANES

    def buffer_rows(cols):
        return cols // LANES * rows + (rest_rows if cols % LANES else 0)

    me = lax.axis_index("tp")
    my_vp = lax.axis_index("vp")
    chip = me // 2
    core = me % 2
    peer = 2 * chip + 1 - core
    turn = 1 - 2 * core

    def chip_at(offset):
        return (chip + offset + chips) % chips

    fwd = 2 * chip_at(turn) + core
    bwd = 2 * chip_at(-turn) + core

    barrier = pltpu.get_barrier_semaphore()
    def tp_peer(j):
        return 2 * chip_at(j // 2) + (core if j % 2 == 0 else 1 - core)

    far_first = sorted(range(1, tp_size), key=lambda j: -min(j // 2, chips - j // 2))
    for j in far_first:
        pl.semaphore_signal(barrier, inc=1, device_id={"tp": tp_peer(j)}, device_id_type=MESH_ID)
    for j in range(1, vp_size):
        pl.semaphore_signal(barrier, inc=1, device_id={"vp": (my_vp + j) % vp_size}, device_id_type=MESH_ID)

    hid_load = pltpu.make_async_copy(hid_hbm, hid, small_sem.at[0])
    tok_load = pltpu.make_async_copy(tok_hbm, tok, small_sem.at[1])
    hid_load.start()
    for i, src in enumerate([g1_hbm, b1_hbm, g2_hbm, b2_hbm]):
        pltpu.make_async_copy(src, norms.at[i], small_sem.at[2]).start()
    tok_load.start()

    def block_of(phase, half, sign):
        if phase == 0:
            return chip_at(2)
        if phase == 3:
            return chip
        if (phase == 1) == (half == 0):
            return chip_at(-sign)
        return chip_at(sign)

    def first_row(phase, half, own):
        if own:
            return (2 * block_of(phase, half, turn) + core) * own_cols + half * half_cols
        return (2 * block_of(phase, half, -turn) + 1 - core) * own_cols + half * half_cols

    def table_load(phase, half, own):
        count = half_cols if half == 0 else own_cols - half_cols
        span = pl.ds(pl.multiple_of(first_row(phase, half, own), 16), count)
        return pltpu.make_async_copy(emb.at[span], e_all.at[span], e_sem.at[min(phase, 1)])

    def wait_table(phases):
        span = pl.ds(0, 2 * own_cols * phases)
        pltpu.make_async_copy(emb.at[span], e_all.at[span], e_sem.at[min(phases - 1, 1)]).wait()

    for half in range(2):
        rows_at = pl.ds(pl.multiple_of(first_row(0, half, 0), 16), HEAD)
        pltpu.make_async_copy(emb.at[rows_at], early_rows.at[pl.ds(half * HEAD, HEAD)], early_sem.at[0]).start()

    hid_load.wait()
    pltpu.make_async_copy(norms, norms, small_sem.at[2]).wait()
    tok_load.wait()
    for phase in range(4):
        for own in range(2):
            for half in range(2):
                table_load(phase, half, own).start()

    def share(src, dst, send, recv, axis, j):
        to = tp_peer(j) if axis == "tp" else (my_vp + j) % vp_size
        return pltpu.make_async_remote_copy(
            src_ref=src, dst_ref=dst.at[j - 1], send_sem=send, recv_sem=recv,
            device_id={axis: to}, device_id_type=MESH_ID)

    def all_shared(dst, send, recv, axis):
        at = (me + 1) % tp_size if axis == "tp" else (my_vp + 1) % vp_size
        return pltpu.make_async_remote_copy(
            src_ref=dst, dst_ref=dst, send_sem=send, recv_sem=recv,
            device_id={axis: at}, device_id_type=MESH_ID)

    def share_stats(s):
        for j in far_first:
            share(stat_src.at[s], stat_in.at[s], stat_send.at[0], stat_recv.at[s], "tp", j).start()

    def stat_total(s):
        all_shared(stat_in.at[s], stat_send.at[0], stat_recv.at[s], "tp").wait_recv()
        total = stat_src[s]
        for j in range(1, tp_size):
            total = total + stat_in[s, j - 1]
        return total

    x = hid[...].astype(jnp.float32)
    stat_src[0] = _row_stats(x)
    pl.semaphore_wait(barrier, tp_size - 1 + vp_size - 1)
    share_stats(0)
    early_out[pl.ds(2 * HEAD, rows), :] = x
    early_out[pl.ds(2 * HEAD + rows, 8), :] = jnp.concatenate(
        [norms[0], norms[1], jnp.zeros((6, width), jnp.float32)], axis=0)
    pltpu.make_async_copy(emb.at[pl.ds(0, 2 * HEAD)], early_rows, early_sem.at[0]).wait()
    early_out[pl.ds(0, 2 * HEAD), :] = early_rows[...].astype(jnp.float32)
    early_copy = pltpu.make_async_remote_copy(
        src_ref=early_out, dst_ref=early_in, send_sem=early_sem.at[1], recv_sem=early_sem.at[2],
        device_id={"tp": peer}, device_id_type=MESH_ID)
    early_copy.start()
    early_copy.wait_recv()
    early_rows[...] = early_in[pl.ds(0, 2 * HEAD), :].astype(jnp.bfloat16)
    mean, rstd = _mean_rstd(stat_total(0), rows, full_width)
    xn[...] = _normalize(x, mean, rstd, norms[0], norms[1])
    xn_peer[...] = _normalize(
        early_in[pl.ds(2 * HEAD, rows), :], mean, rstd,
        early_in[pl.ds(2 * HEAD + rows, 1), :], early_in[pl.ds(2 * HEAD + rows + 1, 1), :])

    def chunk_dot(dst, base, row0, first, cols):
        for c in range(first, cols, DOT_COLS):
            n = min(DOT_COLS, cols - c)
            part = e_all[pl.ds(pl.multiple_of(row0 + c, 16), n), :]
            v = lax.dot_general(xn[...], part, (((1,), (1,)), ((), ())), preferred_element_type=jnp.float32)
            for t in range(0, n, LANES):
                at = base + (c + t) // LANES * rows
                if t + LANES <= n:
                    dst[pl.ds(at, rows), :] = v[:, t : t + LANES]
                else:
                    dst[pl.ds(at, rest_rows), :] = jnp.concatenate(
                        [v[q : q + rest_rows, t:n] for q in range(0, rows, rest_rows)], axis=1)

    def cols_of(half, last):
        return tail if half == 1 and last else CHUNK

    def at_of(phase, half, k):
        return phase * n_chunks + half * half_chunks + k

    own_rows = buffer_rows(own_cols)

    def base_of(phase, half, k):
        return pl.multiple_of(phase * own_rows + (half * half_chunks + k) * buffer_rows(CHUNK), 8)

    def span_of(phase, half, k, last):
        begin = buffer_rows(HEAD) if phase == 0 and isinstance(k, int) and k == 0 else 0
        return pl.ds(base_of(phase, half, k) + begin, buffer_rows(cols_of(half, last)) - begin)

    def peer_recv_of(phase, k):
        return peer_recv.at[k if phase == 0 else half_chunks + phase - 1]

    def peer_copy(phase, half, k, last):
        span = span_of(phase, half, k, last)
        return pltpu.make_async_remote_copy(
            src_ref=to_peer.at[span], dst_ref=from_peer.at[span],
            send_sem=peer_send.at[0], recv_sem=peer_recv_of(phase, k),
            device_id={"tp": peer}, device_id_type=MESH_ID)

    def wait_peer(recv, count):
        ref = from_peer.at[pl.ds(0, count)]
        pltpu.make_async_remote_copy(
            src_ref=ref, dst_ref=ref, send_sem=peer_send.at[0], recv_sem=recv,
            device_id={"tp": peer}, device_id_type=MESH_ID).wait_recv()

    def wait_peer_phase(phase):
        wait_peer(peer_recv_of(phase, 0), own_rows)

    def wait_peer_chunk(k, last):
        wait_peer(peer_recv_of(0, k), sum(span_of(0, half, k, last).size for half in range(2)))

    def ring_recv_of(phase, half, k, last):
        return ring_recv.at[phase if phase < 2 else 2 + k + (half if last else 0)]

    def ring_copy(phase, half, k, last):
        span = span_of(phase, half, k, last)
        forward = (half == 0) != (phase == 1)
        return pltpu.make_async_remote_copy(
            src_ref=mine.at[span], dst_ref=ring.at[span],
            send_sem=ring_send.at[0], recv_sem=ring_recv_of(phase, half, k, last),
            device_id={"tp": fwd if forward else bwd}, device_id_type=MESH_ID)

    def whole_phase(ref, phase):
        return ref.at[pl.ds(phase * own_rows, own_rows)]

    def wait_ring(recv, count):
        ref = ring.at[pl.ds(0, count)]
        pltpu.make_async_remote_copy(
            src_ref=ref, dst_ref=ref, send_sem=ring_send.at[0], recv_sem=recv,
            device_id={"tp": fwd}, device_id_type=MESH_ID).wait_recv()

    def wait_ring_phase(phase):
        wait_ring(ring_recv.at[phase], own_rows)

    def head_ring_copy(half, c):
        span = pl.ds(half * half_chunks * buffer_rows(CHUNK) + buffer_rows(c), buffer_rows(HEAD_STEP))
        return pltpu.make_async_remote_copy(
            src_ref=mine.at[span], dst_ref=ring.at[span],
            send_sem=ring_send.at[0], recv_sem=ring_recv.at[0],
            device_id={"tp": bwd if half else fwd}, device_id_type=MESH_ID)

    def add_into(base, others, begin, end):
        for r in range(begin, end, 8):
            v = mine[pl.ds(base + r, 8), :]
            for ref, at in others:
                v = v + ref[pl.ds(at + r, 8), :]
            mine[pl.ds(base + r, 8), :] = v

    def to_peer_dot(phase, half, k, last, first=0, end=None):
        chunk_dot(to_peer, base_of(phase, half, k), first_row(phase, half, 0) + k * CHUNK,
                  first, end or cols_of(half, last))

    def mine_dot(phase, half, k, last, first=0, end=None):
        if phase < 3:
            dst, base = mine, base_of(phase, half, k)
        else:
            dst, base = z_out, base_of(0, half, k)
        chunk_dot(dst, base, first_row(phase, half, 1) + k * CHUNK, first, end or cols_of(half, last))

    def first_product():
        dims = (((1,), (1,)), ((), ()))
        for c in range(0, HEAD, HEAD_STEP):
            for half in range(2):
                part = e_all[pl.ds(pl.multiple_of(first_row(0, half, 1) + c, 16), HEAD_STEP), :]
                v = lax.dot_general(xn[...], part, dims, preferred_element_type=jnp.float32) + lax.dot_general(
                    xn_peer[...], early_rows[pl.ds(half * HEAD + c, HEAD_STEP), :], dims,
                    preferred_element_type=jnp.float32)
                for t in range(0, HEAD_STEP, LANES):
                    mine[pl.ds(base_of(0, half, 0) + (c + t) // LANES * rows, rows), :] = v[:, t : t + LANES]
            for half in range(2):
                head_ring_copy(half, c).start()
        for half in range(2):
            to_peer_dot(0, half, 0, False, HEAD)
        for half in range(2):
            peer_copy(0, half, 0, False).start()
        for half in range(2):
            mine_dot(0, half, 0, False, HEAD)
        wait_peer_chunk(0, False)
        for half in range(2):
            at = base_of(0, half, 0)
            add_into(at, [(from_peer, at)], buffer_rows(HEAD), buffer_rows(CHUNK))
        for half in range(2):
            ring_copy(0, half, 0, False).start()

    def join(phase, k, last):
        for half in range(2):
            at = base_of(phase, half, k)
            add_into(at, [(from_peer, at)], 0, buffer_rows(cols_of(half, last)))
        for half in range(2):
            ring_copy(phase, half, k, last).start()

    def product(phase, k, last):
        for half in range(2):
            to_peer_dot(phase, half, k, last)
        for half in range(2):
            peer_copy(phase, half, k, last).start()
        for half in range(2):
            mine_dot(phase, half, k, last)
        if phase == 0:
            wait_peer_chunk(k, last)
            join(phase, k, last)

    def each_chunk(body, begin=0):
        def step(k, carry):
            body(k, False)
            return carry

        for k in range(begin, 1):
            body(k, False)
        lax.fori_loop(1, half_chunks - 1, step, 0)
        body(half_chunks - 1, True)

    wait_table(1)
    first_product()
    each_chunk(functools.partial(product, 0), 1)

    wait_table(3)

    def pick_rows():
        wanted = tok[...].astype(jnp.float32) - (my_vp * vocab_rows).astype(jnp.float32)
        wanted = jnp.concatenate([wanted, jnp.zeros((1, LANES - rows), jnp.float32)], axis=1)
        wanted = _as_columns(wanted)[:rows].astype(jnp.int32)
        lane = lax.broadcasted_iota(jnp.int32, wanted.shape, 1)

        def add(first, count):
            hits = []
            for c in range(0, count, LANES):
                hits.append(jnp.where(lane + (first + c) == wanted, 1.0, 0.0).astype(jnp.bfloat16))
            e_src[...] += jnp.dot(
                jnp.concatenate(hits, axis=1), e_all[pl.ds(pl.multiple_of(first, LANES), count), :],
                preferred_element_type=jnp.float32)

        def step(i, carry):
            add(i * PICK, PICK)
            return carry

        e_src[...] = jnp.zeros_like(e_src)
        lax.fori_loop(0, vocab_rows // PICK, step, 0)
        if vocab_rows % PICK:
            add(vocab_rows // PICK * PICK, vocab_rows % PICK)

    each_chunk(functools.partial(product, 1))
    wait_peer_phase(1)
    each_chunk(functools.partial(join, 1))
    pick_rows()
    for j in range(1, vp_size):
        share(e_src, e_in, row_sem.at[0], row_sem.at[1], "vp", j).start()
    each_chunk(functools.partial(product, 2))

    def token_rows():
        rows_sum = e_src[...]
        for j in range(1, vp_size):
            rows_sum = rows_sum + e_in[j - 1]
        return rows_sum

    all_shared(e_in, row_sem.at[0], row_sem.at[1], "vp").wait()
    stat_src[1] = _row_stats(token_rows())
    share_stats(1)

    def forward_chunk(k, last):
        for half in range(2):
            at = base_of(2, half, k)
            add_into(at, [(from_peer, at), (ring, base_of(0, half, k))], 0, buffer_rows(cols_of(half, last)))
        for half in range(2):
            ring_copy(2, half, k, last).start()

    wait_peer_phase(2)
    wait_ring_phase(0)
    each_chunk(forward_chunk)
    each_chunk(functools.partial(product, 3))
    mean, rstd = _mean_rstd(stat_total(1), rows, full_width)
    nin_out[...] = _normalize(token_rows(), mean, rstd, norms[2], norms[3])

    top[...] = jnp.full(top.shape, jnp.finfo(jnp.float32).min, jnp.float32)
    acc[...] = jnp.zeros_like(acc)

    def finish_chunk(k, last):
        for half in range(2):
            cols = cols_of(half, last)
            base, peer_base = base_of(0, half, k), base_of(3, half, k)
            single, chain = base_of(1, half, k), base_of(2, half, k)
            if last:
                ring_copy(2, half, k, last).wait_recv()
            elif half == 0:
                wait_ring(ring_recv_of(2, 0, k, False), 2 * buffer_rows(CHUNK))

            def final(r):
                v = (z_out[pl.ds(base + r, 8), :] + from_peer[pl.ds(peer_base + r, 8), :]) + (
                    ring[pl.ds(single + r, 8), :] + ring[pl.ds(chain + r, 8), :])
                z_out[pl.ds(base + r, 8), :] = v
                return v

            full = cols // LANES
            if cols % LANES:
                packed = jnp.concatenate([final(full * rows + r) for r in range(0, rest_rows, 8)], axis=0)
            for r in range(0, rows, 8):
                tiles = [final(t * rows + r) for t in range(full)]
                if cols % LANES:
                    v = _unpacked(packed, r, rest_rows, rest)
                    tiles.append(jnp.where(lax.broadcasted_iota(jnp.int32, v.shape, 1) < rest, v, -jnp.inf))
                old = top[r : r + 8, :]
                best = functools.reduce(jnp.maximum, tiles, old)
                total = acc[r : r + 8, :] * jnp.exp(old - best)
                for v in tiles:
                    total = total + jnp.exp(v - best)
                top[r : r + 8, :] = best
                acc[r : r + 8, :] = total

    wait_peer_phase(3)
    wait_ring_phase(1)
    each_chunk(finish_chunk)

    tops = jnp.concatenate([top[...], top[...]], axis=0).T
    sums = jnp.concatenate([acc[...], acc[...]], axis=0).T
    best = jnp.max(tops, axis=0, keepdims=True)
    total = jnp.sum(sums * jnp.exp(tops - best), axis=0, keepdims=True)

    def merge(best, total, other):
        tops = [best] + [other[j, 0:1, :] for j in range(other.shape[0])]
        sums = [total] + [other[j, 1:2, :] for j in range(other.shape[0])]
        new = functools.reduce(jnp.maximum, tops)
        return new, functools.reduce(jnp.add, [t * jnp.exp(b - new) for b, t in zip(tops, sums)])

    vp_far_first = sorted(range(1, vp_size), key=lambda j: -min(j, vp_size - j))
    stages = (
        ("tp", far_first, lse_in.at[pl.ds(0, tp_size - 1)]),
        ("vp", vp_far_first, lse_in.at[pl.ds(tp_size - 1, vp_size - 1)]))
    for i, (axis, order, other) in enumerate(stages):
        lse_src[i, 0:1, :] = best
        lse_src[i, 1:2, :] = total
        for j in order:
            share(lse_src.at[i], other, lse_send.at[0], lse_recv.at[i], axis, j).start()
        all_shared(other, lse_send.at[0], lse_recv.at[i], axis).wait_recv()
        best, total = merge(best, total, other)
    ls_out[...] = jnp.broadcast_to(best + jnp.log(total), ls_out.shape)

    early_copy.wait_send()
    all_shared(stat_in, stat_send.at[0], stat_recv.at[0], "tp").wait_send()
    all_shared(lse_in, lse_send.at[0], lse_recv.at[0], "tp").wait_send()
    sent_to_peer = to_peer.at[pl.ds(0, 4 * own_rows - 2 * buffer_rows(HEAD))]
    for ref, sem in ((mine, ring_send), (sent_to_peer, peer_send)):
        pltpu.make_async_remote_copy(
            src_ref=ref, dst_ref=ref, send_sem=sem.at[0], recv_sem=ring_recv.at[0],
            device_id={"tp": peer}, device_id_type=MESH_ID).wait_send()


def _subtract_kernel(z, ls, nin, logprobs, log_sum, next_in, out, sums, sems):
    rows, n = out.shape
    rest = n % LANES
    rest_rows = rows * rest // LANES
    step = rows // 4
    copies = [
        pltpu.make_async_copy(nin, next_in, sems.at[4]),
        pltpu.make_async_copy(sums, log_sum, sems.at[5]),
    ]
    copies[0].start()
    sums[...] = ls[0:1, :rows]
    cols = _as_columns(ls[0:1, :])[:rows]
    packed = z[n // LANES * rows :, :]
    for i in range(4):
        for r in range(i * step, (i + 1) * step, 8):
            for t in range(n // LANES):
                out[r : r + 8, t * LANES : (t + 1) * LANES] = z[t * rows + r : t * rows + r + 8, :] - cols[r : r + 8]
            if rest:
                v = _unpacked(packed, r, rest_rows, rest) - cols[r : r + 8]
                out[r : r + 8, n - rest :] = v[:, :rest]
        span = pl.ds(i * step, step)
        copies.append(pltpu.make_async_copy(out.at[span], logprobs.at[span], sems.at[i]))
        copies[-1].start()
        if i == 0:
            copies[1].start()
    for copy in copies:
        copy.wait()


def solution(mesh):
    tp_size = mesh.shape["tp"]
    vp_size = mesh.shape["vp"]

    def per_device(hidden, lnf_gain, lnf_bias, emb_table, next_tok, eln_gain, eln_bias):
        rows, width = hidden.shape
        own_cols = emb_table.shape[0] // tp_size
        n_chunks = pl.cdiv(own_cols, CHUNK)
        f32 = jnp.float32
        vmem = pl.BlockSpec(memory_space=pltpu.VMEM)
        hbm = pl.BlockSpec(memory_space=pltpu.HBM)
        dma = pltpu.SemaphoreType.DMA
        own_rows = rows * own_cols // LANES
        z, ls, nin = pl.pallas_call(
            functools.partial(_head_kernel, tp_size, vp_size),
            out_shape=(
                pltpu.VMEM((own_rows, LANES), f32),
                pltpu.VMEM((8, LANES), f32),
                pltpu.VMEM((rows, width), jnp.bfloat16),
            ),
            in_specs=[hbm] * 7,
            out_specs=(vmem,) * 3,
            scratch_shapes=[
                pltpu.VMEM((rows, width), hidden.dtype),
                pltpu.VMEM((4, 1, width), f32),
                pltpu.VMEM((1, rows), jnp.int32),
                pltpu.VMEM(emb_table.shape, emb_table.dtype),
                pltpu.VMEM((3 * own_rows, LANES), f32),
                pltpu.VMEM((4 * own_rows, LANES), f32),
                pltpu.VMEM((4 * own_rows, LANES), f32),
                pltpu.VMEM((3 * own_rows, LANES), f32),
                pltpu.VMEM((rows, width), jnp.bfloat16),
                pltpu.VMEM((rows, width), jnp.bfloat16),
                pltpu.VMEM((2 * HEAD + rows + 8, width), f32),
                pltpu.VMEM((2 * HEAD + rows + 8, width), f32),
                pltpu.VMEM((2 * HEAD, width), emb_table.dtype),
                pltpu.VMEM((rows, LANES), f32),
                pltpu.VMEM((rows, LANES), f32),
                pltpu.VMEM((rows, width), f32),
                pltpu.VMEM((vp_size - 1, rows, width), f32),
                pltpu.VMEM((2, 1, LANES), f32),
                pltpu.VMEM((2, tp_size - 1, 1, LANES), f32),
                pltpu.VMEM((2, 2, LANES), f32),
                pltpu.VMEM((tp_size - 1 + vp_size - 1, 2, LANES), f32),
                dma((3,)),
                dma((2,)),
                dma((3,)),
                dma((1,)),
                dma((n_chunks // 2 + 3,)),
                dma((1,)),
                dma((2 + n_chunks // 2 + 1,)),
                dma((1,)),
                dma((2,)),
                dma((2,)),
                dma((1,)),
                dma((2,)),
            ],
            compiler_params=pltpu.CompilerParams(
                collective_id=0, has_side_effects=True, vmem_limit_bytes=64_500_000),
            name="vocab_head",
        )(
            hidden, lnf_gain.reshape(1, width), lnf_bias.reshape(1, width),
            eln_gain.reshape(1, width), eln_bias.reshape(1, width), next_tok.reshape(1, rows), emb_table,
        )
        logprobs, log_sum, next_in = pl.pallas_call(
            _subtract_kernel,
            out_shape=(
                jax.ShapeDtypeStruct((rows, own_cols), f32),
                jax.ShapeDtypeStruct((1, rows), f32),
                jax.ShapeDtypeStruct((rows, width), jnp.bfloat16),
            ),
            in_specs=[vmem] * 3,
            out_specs=(hbm,) * 3,
            scratch_shapes=[pltpu.VMEM((rows, own_cols), f32), pltpu.VMEM((1, rows), f32), dma((6,))],
            compiler_params=pltpu.CompilerParams(vmem_limit_bytes=16_000_000),
            name="log_probs",
        )(z, ls, nin)
        return logprobs, log_sum.reshape(rows), next_in

    return jax.shard_map(
        per_device,
        mesh=mesh,
        in_specs=(P("dp", "tp"), P("tp"), P("tp"), P("vp", "tp"), P("dp"), P("tp"), P("tp")),
        out_specs=(P("dp", ("vp", "tp")), P("dp"), P("dp", "tp")),
        check_vma=False,
    )
```
